64 devices in a mesh: dp: 4 (over x, y), gp: 16 (over z, core).
Axes of the slice: x: 2, y: 2, z: 8, core: 2. Of those that a mesh axis runs over, the one named last changes fastest.
The devices are a block of a 4x4x8 slice.
Arguments:
- x_prev: float32 [65536, 227], P(('dp', 'gp')), parts along dimension 0
- x_cur: float32 [65536, 227], P(('dp', 'gp')), parts along dimension 0
- forcing: float32 [65536, 2, 5], P(('dp', 'gp')), parts along dimension 0
- grid_static: float32 [65536, 5], P(('dp', 'gp')), parts along dimension 0
- g2m_feat: float32 [65536, 4], P(('dp', 'gp')), parts along dimension 0
- m2g_feat: float32 [65536, 4], P(('dp', 'gp')), parts along dimension 0
- mesh_feat: float32 [32768, 3], P(('dp', 'gp')), parts along dimension 0
- mesh_edge_feat: float32 [32768, 6, 4], P(('dp', 'gp')), parts along dimension 0
- norm_stats: float32 [4, 227], replicated
- w_grid_in: bfloat16 [464, 512], replicated
- w_mesh_in: bfloat16 [3, 512], replicated
- w_eemb_in: bfloat16 [3, 4, 512], replicated
- w_embed_out: bfloat16 [5, 512, 512], replicated
- w_edge_in: bfloat16 [18, 1536, 512], replicated
- w_edge_out: bfloat16 [18, 512, 512], replicated
- w_node_in: bfloat16 [18, 1024, 512], replicated
- w_node_out: bfloat16 [18, 512, 512], replicated
- w_grid_self: bfloat16 [2, 512, 512], replicated
- w_out_hidden: bfloat16 [512, 512], replicated
- w_out_final: bfloat16 [512, 227], replicated
Outputs:
- output 1: float32 [65536, 227], P(('dp', 'gp')), parts along dimension 0
- output 2: float32 [65536, 227], P(('dp', 'gp')), parts along dimension 0
There are 4 independent parts. The reference program is written for one: setup_inputs(seed, part) draws one part's arguments, and reference() takes and returns one part's arrays. A program takes and returns all parts, laid end to end along the dimension named above; an argument that names none is the same for every part.
All inputs are finite; a program needn't handle non-finite values.
Results may differ from the reference program's by a relative error of at most 0.00827091.
Values are sent between devices in bfloat16 or wider.
A program may use at most 768 MiB of HBM per device.

```python
import jax
import jax.numpy as jnp
from jax import lax

GRID_NODES = 16384
MESH_NODES = 8192
SHIFT = 256
LATENT = 512
VARS = 227
FORCE = 5
STATIC = 5
LAYERS = 16
EDGE_FEAT = 4
MESH_FEAT = 3
OFFSET_COUNT = 6

GRID_RATIO = GRID_NODES // MESH_NODES
QUARTER = MESH_NODES // 4
BLOCKS = LAYERS + 2
IN_FEAT = 2 * VARS + FORCE + STATIC
OFFSETS = (1, -1, SHIFT, -SHIFT, QUARTER, -QUARTER)


def normal_weight(key_in, out_shape, fan_in):
    return (jax.random.normal(key_in, out_shape, jnp.float32) * fan_in ** -0.5).astype(jnp.bfloat16)


def setup_inputs(seed: int = 0, part: int = 0) -> dict:
    root_key = jax.random.key(seed)
    part_keys = jax.random.split(jax.random.fold_in(root_key, part), 8)
    weight_keys = jax.random.split(jax.random.key(seed + 1), 15)
    norm_stats = jnp.stack([
        0.5 * jax.random.normal(weight_keys[0], (VARS,), jnp.float32),
        jax.random.uniform(weight_keys[1], (VARS,), jnp.float32, 0.5, 1.5),
        0.2 * jax.random.normal(weight_keys[2], (VARS,), jnp.float32),
        jax.random.uniform(weight_keys[3], (VARS,), jnp.float32, 0.2, 0.6)])
    return {
        "x_prev": jax.random.normal(part_keys[0], (GRID_NODES, VARS), jnp.float32),
        "x_cur": jax.random.normal(part_keys[1], (GRID_NODES, VARS), jnp.float32),
        "forcing": jax.random.normal(part_keys[2], (GRID_NODES, 2, FORCE), jnp.float32),
        "grid_static": jax.random.normal(part_keys[3], (GRID_NODES, STATIC), jnp.float32),
        "g2m_feat": jax.random.normal(part_keys[4], (GRID_NODES, EDGE_FEAT), jnp.float32),
        "m2g_feat": jax.random.normal(part_keys[5], (GRID_NODES, EDGE_FEAT), jnp.float32),
        "mesh_feat": jax.random.normal(part_keys[6], (MESH_NODES, MESH_FEAT), jnp.float32),
        "mesh_edge_feat": jax.random.normal(part_keys[7], (MESH_NODES, OFFSET_COUNT, EDGE_FEAT), jnp.float32),
        "norm_stats": norm_stats,
        "w_grid_in": normal_weight(weight_keys[4], (IN_FEAT, LATENT), IN_FEAT),
        "w_mesh_in": normal_weight(weight_keys[5], (MESH_FEAT, LATENT), MESH_FEAT),
        "w_eemb_in": normal_weight(weight_keys[6], (3, EDGE_FEAT, LATENT), EDGE_FEAT),
        "w_embed_out": normal_weight(weight_keys[7], (5, LATENT, LATENT), LATENT),
        "w_edge_in": normal_weight(weight_keys[8], (BLOCKS, 3 * LATENT, LATENT), 3 * LATENT),
        "w_edge_out": normal_weight(weight_keys[9], (BLOCKS, LATENT, LATENT), LATENT),
        "w_node_in": normal_weight(weight_keys[10], (BLOCKS, 2 * LATENT, LATENT), 2 * LATENT),
        "w_node_out": normal_weight(weight_keys[11], (BLOCKS, LATENT, LATENT), LATENT),
        "w_grid_self": normal_weight(weight_keys[12], (2, LATENT, LATENT), LATENT),
        "w_out_hidden": normal_weight(weight_keys[13], (LATENT, LATENT), LATENT),
        "w_out_final": normal_weight(weight_keys[14], (LATENT, VARS), LATENT),
    }


def layer_norm(values):
    centre = jnp.mean(values, axis=-1, keepdims=True)
    centred = values - centre
    spread = jnp.mean(centred * centred, axis=-1, keepdims=True)
    return centred * lax.rsqrt(spread + 1e-5)


def matmul_f32(values, weight):
    return jnp.dot(values, weight, preferred_element_type=jnp.float32)


def mlp_tail(pre_act, w_second):
    hidden = jax.nn.silu(pre_act).astype(jnp.bfloat16)
    return layer_norm(matmul_f32(hidden, w_second))


def residual(base, update):
    return (base.astype(jnp.float32) + update).astype(jnp.bfloat16)


def embed_static(features, w_first, w_second):
    return mlp_tail(matmul_f32(features.astype(jnp.bfloat16), w_first), w_second).astype(jnp.bfloat16)


def reference(x_prev, x_cur, forcing, grid_static, g2m_feat, m2g_feat, mesh_feat, mesh_edge_feat, norm_stats, w_grid_in, w_mesh_in, w_eemb_in, w_embed_out, w_edge_in, w_edge_out, w_node_in, w_node_out, w_grid_self, w_out_hidden, w_out_final):
    mesh_lat = embed_static(mesh_feat, w_mesh_in, w_embed_out[1])
    g2m_lat = embed_static(g2m_feat, w_eemb_in[0], w_embed_out[2])
    m2g_lat = embed_static(m2g_feat, w_eemb_in[1], w_embed_out[3])
    edge_base = embed_static(mesh_edge_feat.reshape(MESH_NODES * OFFSET_COUNT, EDGE_FEAT), w_eemb_in[2], w_embed_out[4])
    in_mean = norm_stats[0]
    in_std = norm_stats[1]
    diff_mean = norm_stats[2]
    diff_std = norm_stats[3]

    def proc_layer(layer_state, layer_weights):
        mesh_cur, edge_lat = layer_state
        w_edge, w_edge_two, w_node, w_node_two = layer_weights
        send_proj = matmul_f32(mesh_cur, w_edge[LATENT:2 * LATENT])
        send_term = jnp.stack([jnp.roll(send_proj, -offset, axis=0) for offset in OFFSETS], axis=1).reshape(MESH_NODES * OFFSET_COUNT, LATENT)
        recv_term = matmul_f32(mesh_cur, w_edge[2 * LATENT:])
        pre_act = matmul_f32(edge_lat, w_edge[:LATENT]) + send_term
        pre_act = (pre_act.reshape(MESH_NODES, OFFSET_COUNT, LATENT) + recv_term[:, None, :]).reshape(MESH_NODES * OFFSET_COUNT, LATENT)
        edge_lat = residual(edge_lat, mlp_tail(pre_act, w_edge_two))
        edge_sum = jnp.sum(edge_lat.reshape(MESH_NODES, OFFSET_COUNT, LATENT).astype(jnp.float32), axis=1).astype(jnp.bfloat16)
        mesh_cur = residual(mesh_cur, mlp_tail(matmul_f32(mesh_cur, w_node[:LATENT]) + matmul_f32(edge_sum, w_node[LATENT:]), w_node_two))
        return (mesh_cur, edge_lat), None

    def forecast_step(state_pair, force_now):
        state_prev, state_cur = state_pair
        features = jnp.concatenate([(state_prev - in_mean) / in_std, (state_cur - in_mean) / in_std, force_now, grid_static], axis=1)
        grid_lat = embed_static(features, w_grid_in, w_embed_out[0])
        w_first = w_edge_in[0]
        senders = jnp.roll(grid_lat, SHIFT * GRID_RATIO, axis=0)
        recv_term = matmul_f32(mesh_lat, w_first[2 * LATENT:])
        pre_act = matmul_f32(g2m_lat, w_first[:LATENT]) + matmul_f32(senders, w_first[LATENT:2 * LATENT])
        pre_act = (pre_act.reshape(MESH_NODES, GRID_RATIO, LATENT) + recv_term[:, None, :]).reshape(GRID_NODES, LATENT)
        enc_edge = residual(g2m_lat, mlp_tail(pre_act, w_edge_out[0]))
        enc_sum = jnp.sum(enc_edge.reshape(MESH_NODES, GRID_RATIO, LATENT).astype(jnp.float32), axis=1).astype(jnp.bfloat16)
        node_first = w_node_in[0]
        mesh_cur = residual(mesh_lat, mlp_tail(matmul_f32(mesh_lat, node_first[:LATENT]) + matmul_f32(enc_sum, node_first[LATENT:]), w_node_out[0]))
        grid_cur = residual(grid_lat, mlp_tail(matmul_f32(grid_lat, w_grid_self[0]), w_grid_self[1]))
        layer_weights = (w_edge_in[1:BLOCKS - 1], w_edge_out[1:BLOCKS - 1], w_node_in[1:BLOCKS - 1], w_node_out[1:BLOCKS - 1])
        layer_out, no_stack = lax.scan(proc_layer, (mesh_cur, edge_base), layer_weights)
        mesh_cur = layer_out[0]
        w_last = w_edge_in[BLOCKS - 1]
        send_term = matmul_f32(jnp.roll(mesh_cur, -SHIFT, axis=0), w_last[LATENT:2 * LATENT])
        pre_act = matmul_f32(m2g_lat, w_last[:LATENT]) + matmul_f32(grid_cur, w_last[2 * LATENT:])
        pre_act = (pre_act.reshape(MESH_NODES, GRID_RATIO, LATENT) + send_term[:, None, :]).reshape(GRID_NODES, LATENT)
        dec_edge = residual(m2g_lat, mlp_tail(pre_act, w_edge_out[BLOCKS - 1]))
        node_last = w_node_in[BLOCKS - 1]
        grid_out = residual(grid_cur, mlp_tail(matmul_f32(grid_cur, node_last[:LATENT]) + matmul_f32(dec_edge, node_last[LATENT:]), w_node_out[BLOCKS - 1]))
        hidden = jax.nn.silu(matmul_f32(grid_out, w_out_hidden)).astype(jnp.bfloat16)
        prediction = matmul_f32(hidden, w_out_final)
        state_next = state_cur + diff_std * prediction + diff_mean
        return (state_cur, state_next), state_next

    final_pair, stacked = lax.scan(forecast_step, (x_prev, x_cur), jnp.swapaxes(forcing, 0, 1))
    return stacked[0], stacked[1]
```

```python
import functools

import jax
import jax.numpy as jnp
from jax import lax
from jax.experimental import pallas as pl
from jax.experimental.pallas import tpu as pltpu
from jax.sharding import PartitionSpec as P

F32 = jnp.float32
BF16 = jnp.bfloat16
SLAB = 16
RATIO = 2
OFFSETS = 6


def dot(a, b):
    return jnp.dot(a, b, preferred_element_type=F32)


def dot_t(a, b):
    return lax.dot_general(a, b, (((0,), (0,)), ((), ())), preferred_element_type=F32)


def dot_bt(a, b):
    return lax.dot_general(a, b, (((1,), (1,)), ((), ())), preferred_element_type=F32)


def silu(x):
    half = 0.5 * x
    return half * jnp.tanh(half) + half


def layer_norm(y):
    centred = y - jnp.mean(y, axis=-1, keepdims=True)
    spread = jnp.mean(centred * centred, axis=-1, keepdims=True)
    return centred * lax.rsqrt(spread + 1e-5)


def kernel(cfg, *refs):
    names = cfg["names"]
    r = dict(zip(names, refs, strict=True))
    n, rows, latent, shift, layers = cfg["n"], cfg["rows"], cfg["latent"], cfg["shift"], cfg["layers"]
    nvar, in_feat = cfg["nvar"], cfg["in_feat"]
    cols_j = n * rows // shift
    nblk = shift // n
    quarter = cols_j // 4
    grid_rows = RATIO * rows
    per_blk = OFFSETS * cols_j
    bpc = 2
    chunk = bpc * per_blk
    nchunk = nblk // bpc
    order = [(p + 1) % nblk for p in range(nblk)]
    me = lax.axis_index("gp")
    left = lax.rem(me + n - 1, n)
    right = lax.rem(me + 1, n)
    pre, hid, ys = (r["p0"], r["p1"]), (r["h0"], r["h1"]), (r["y0"], r["y1"])

    def remote(src, dst, send, recv, dev):
        return pltpu.make_async_remote_copy(src_ref=src, dst_ref=dst, send_sem=send, recv_sem=recv, device_id={"gp": dev}, device_id_type=pl.DeviceIdType.MESH)

    last = layers + 1
    loads = {
        "xp": (r["xp_h"], r["xs"].at[0]),
        "xc": (r["xc_h"], r["xs"].at[1]),
        "fs": (r["fs_h"], r["fs"]),
        "ns": (r["ns_h"], r["ns"]),
        "gm": (r["gm_h"], r["gm"]),
        "mf": (r["mf_h"], r["mf"]),
        "ew": (r["ew_h"], r["ew"]),
        "wg": (r["wg_h"], r["wg"].at[0:in_feat]),
        "wemb": (r["wemb_h"], r["wemb"]),
        "wi0": (r["wei_h"].at[0], r["wi"].at[0]),
        "wo0": (r["weo_h"].at[0], r["wo"].at[0]),
        "ni0": (r["wni_h"].at[0], r["ni"].at[0]),
        "no0": (r["wno_h"].at[0], r["no"].at[0]),
        "wself": (r["wself_h"], r["wself"]),
        "wi1": (r["wei_h"].at[last], r["wi"].at[1]),
        "wo1": (r["weo_h"].at[last], r["wo"].at[1]),
        "ni1": (r["wni_h"].at[last], r["ni"].at[1]),
        "no1": (r["wno_h"].at[last], r["no"].at[1]),
        "woh": (r["woh_h"], r["woh"]),
        "wof": (r["wof_h"], r["wof"]),
    }
    loads = {key: pltpu.make_async_copy(src, dst, r["load_sem"].at[i]) for i, (key, (src, dst)) in enumerate(loads.items())}

    def fetch(layer, slot):
        pairs = ((r["wei_h"], r["lwi"]), (r["weo_h"], r["lwo"]), (r["wni_h"], r["lni"]), (r["wno_h"], r["lno"]))
        return [pltpu.make_async_copy(src.at[layer], dst.at[slot], r["fetch_sem"].at[slot, i]) for i, (src, dst) in enumerate(pairs)]

    for key in ("gm", "mf", "ew", "xp", "xc", "fs", "ns", "wg", "wemb", "wi0", "wo0", "ni0", "no0", "wself", "wi1", "wo1", "ni1", "no1", "woh", "wof"):
        loads[key].start()
    for c in fetch(1, 0):
        c.start()

    barrier = pltpu.get_barrier_semaphore()
    for off in range(1, n):
        pl.semaphore_signal(barrier, inc=1, device_id={"gp": lax.rem(me + off, n)}, device_id_type=pl.DeviceIdType.MESH)

    def iota(shape, dim):
        return lax.broadcasted_iota(jnp.int32, shape, dim)

    def onehot(pred):
        return jnp.where(pred, 1.0, 0.0).astype(BF16)

    def perm(shape, slot_dim):
        slot, row = iota(shape, slot_dim), iota(shape, 1 - slot_dim)
        jp = lax.rem(lax.rem(row, cols_j) + (cols_j - 1), cols_j)
        return onehot(slot == jp * nblk + lax.div(row, cols_j))

    for t in range(rows // 128):
        sl = slice(128 * t, 128 * t + 128)
        slot, row = iota((128, rows), 1), iota((128, rows), 0) + 128 * t
        jp = lax.rem(lax.rem(row, cols_j) + (cols_j - 1), cols_j)
        r["pfwd"][sl, :] = onehot(slot == jp * nblk + lax.div(row, cols_j))
        slot, row = iota((128, rows), 0) + 128 * t, iota((128, rows), 1)
        jp = lax.rem(lax.rem(row, cols_j) + (cols_j - 1), cols_j)
        r["pbwd"][sl, :] = onehot(slot == jp * nblk + lax.div(row, cols_j))
    half = rows // 2
    r["ex"][...] = onehot(lax.div(iota((rows, half), 0), RATIO) == iota((rows, half), 1))
    r["ps"][...] = onehot(iota((half, rows), 0) == lax.div(iota((half, rows), 1), RATIO))
    r["wg"][in_feat:, :] = jnp.zeros((r["wg"].shape[0] - in_feat, latent), BF16)

    def act(p, count, hidden, add=None):
        for o in range(0, count, SLAB):
            x = p[o:o + SLAB, :]
            if add is not None:
                x = x + add(o)
            hidden[o:o + SLAB, :] = silu(x).astype(BF16)

    def finish(y, count, store):
        for o in range(0, count, SLAB):
            store(o, layer_norm(y[o:o + SLAB, :]))

    loads["gm"].wait()
    loads["mf"].wait()
    loads["ew"].wait()
    eye = onehot(iota((32, 128), 0) == iota((32, 128), 1))
    r["feat"][...] = dot_t(r["mf"][0:32, :], eye).astype(BF16).reshape(2, half, 128)
    pl.semaphore_wait(barrier, n - 1)

    def feat_copy(off, jj, dev, owner):
        slot = lax.rem(2 * owner + jj + cols_j - 1, cols_j)
        return remote(r["feat"].at[jj, pl.ds(pl.multiple_of(nblk * dev, nblk), nblk), :], r["fin"].at[slot], r["fsend"].at[off, jj], r["frecv"].at[off, jj], dev)

    nb_copies = [
        remote(r["mf"].at[32:48, 0:half], r["mfp"].at[:, half:], r["nsend"].at[0], r["nrecv"].at[0], left),
        remote(r["gm"].at[0, :, 0:rows], r["g2p"].at[:, rows:], r["nsend"].at[1], r["nrecv"].at[1], left),
    ]
    for c in nb_copies:
        c.start()
    for off in range(1, n):
        for jj in range(2):
            feat_copy(off, jj, lax.rem(me + off, n), me).start()
    for jj in range(2):
        r["fin"][lax.rem(2 * me + jj + cols_j - 1, cols_j)] = r["feat"][jj, pl.ds(pl.multiple_of(nblk * me, nblk), nblk), :]
    r["mfp"][:, 0:half] = r["mf"][32:48, half:]
    r["g2p"][:, 0:rows] = r["gm"][0, :, rows:]

    loads["wemb"].wait()

    def embed(lhs_t, w_first, w_second, store):
        pre[0][0:rows, :] = dot_t(lhs_t, w_first)
        act(pre[0], rows, hid[0])
        ys[0][0:rows, :] = dot(hid[0][0:rows, :], w_second)
        finish(ys[0], rows, store)

    loads["wi1"].wait()

    def m2g_body(q, _):
        base = pl.multiple_of(q * rows, rows)

        def store(o, v):
            r["m2g"][pl.ds(base + o, SLAB), :] = v.astype(BF16)

        embed(r["gm"][1, :, pl.ds(base, rows)], r["ew"][2], r["wemb"][3], store)
        r["decst"][pl.ds(base, rows), :] = dot(r["m2g"][pl.ds(base, rows), :], r["wi"][1, 0:latent, :])
        return 0

    lax.fori_loop(0, RATIO, m2g_body, 0)

    for c in nb_copies:
        c.wait()
    loads["wi0"].wait()
    loads["ni0"].wait()

    def store_mesh(o, v):
        r["mlat"][o:o + SLAB, :] = v.astype(BF16)

    embed(r["mfp"][...], r["ew"][0], r["wemb"][1], store_mesh)
    r["nodst"][...] = dot(r["mlat"][...], r["ni"][0, 0:latent, :])

    def g2m_body(q, _):
        base = pl.multiple_of(q * rows, rows)
        hbase = pl.multiple_of(q * half, half)

        def store(o, v):
            r["g2m"][pl.ds(base + o, SLAB), :] = v.astype(BF16)

        embed(r["g2p"][:, pl.ds(base, rows)], r["ew"][1], r["wemb"][2], store)
        hid[1][0:rows, :] = dot(r["ex"][...], r["mlat"][pl.ds(hbase, half), :]).astype(BF16)
        r["encst"][pl.ds(base, rows), :] = dot(r["g2m"][pl.ds(base, rows), :], r["wi"][0, 0:latent, :]) + dot(hid[1][0:rows, :], r["wi"][0, 2 * latent:, :])
        return 0

    lax.fori_loop(0, RATIO, g2m_body, 0)

    for off in range(1, n):
        for jj in range(2):
            feat_copy(off, jj, lax.rem(me + off, n), lax.rem(me + n - off, n)).wait()
    r["featm"][...] = dot(r["pfwd"][...], r["fin"][...].reshape(rows, 128)).astype(BF16)

    def edge_body(k, _):
        sel = onehot(iota((128, 16), 0) == iota((128, 16), 1) + 4 * k)
        sel = jnp.where(iota((128, 16), 1) < 4, sel, jnp.zeros_like(sel))
        w_k = dot(sel, r["ew"][3]).astype(BF16)
        pre[0][0:rows, :] = dot(r["featm"][...], w_k)
        act(pre[0], rows, hid[0])
        ys[0][0:rows, :] = dot(hid[0][0:rows, :], r["wemb"][4])

        def store(o, v):
            pos = order.index(o // cols_j)
            at = pl.multiple_of(pos * per_blk + k * cols_j + o % cols_j, SLAB)
            r["ebase"][pl.ds(at, SLAB), :] = v.astype(BF16)

        finish(ys[0], rows, store)
        return 0

    lax.fori_loop(0, OFFSETS, edge_body, 0)

    for key in ("xp", "xc", "fs", "ns", "wg", "wo0", "no0", "wself", "wo1", "ni1", "no1", "woh", "wof"):
        loads[key].wait()

    def to_blocks(off, dev, owner):
        return remote(r["mcur"].at[:, pl.ds(pl.multiple_of(nblk * dev, nblk), nblk), :], r["hin"].at[pl.ds(2 * owner, 2)], r["asend"].at[off], r["arecv"].at[off], dev)

    def to_grid(off, dev, owner):
        return remote(r["yout"].at[pl.ds(2 * dev, 2)], r["hb"].at[:, pl.ds(pl.multiple_of(nblk * owner, nblk), nblk), :], r["bsend"].at[off], r["brecv"].at[off], dev)

    def layer_body(it, slot0):
        slot = lax.rem(it + slot0, 2)
        par = slot
        for c in fetch(it + 1, slot):
            c.wait()
        for c in fetch(jnp.where(it + 1 < layers, it + 2, 1), 1 - slot):
            c.start()
        wi, wo, ni, no = r["lwi"].at[slot], r["lwo"].at[slot], r["lni"].at[slot], r["lno"].at[slot]
        s0, sup, sdn, rr, n1, e, h = r["s0"], r["sup"], r["sdn"], r["rr"], r["n1"], r["e"], r["h"]
        hv = h[...]
        s0[cols_j:cols_j + rows, :] = dot(hv, wi[latent:2 * latent, :])
        rr[...] = dot(hv, wi[2 * latent:, :])
        n1[...] = dot(hv, ni[0:latent, :])
        for b in range(nblk):
            blk = s0[(b + 1) * cols_j:(b + 2) * cols_j, :]
            sup[b * cols_j:(b + 1) * cols_j, :] = jnp.concatenate([blk[1:], blk[:1]], axis=0)
            sdn[b * cols_j:(b + 1) * cols_j, :] = jnp.concatenate([blk[-1:], blk[:-1]], axis=0)
        halo = [
            remote(s0.at[nblk * cols_j:(nblk + 1) * cols_j], r["halo"].at[par, 0], r["hsend"].at[0], r["hrecv"].at[par, 0], right),
            remote(s0.at[cols_j:2 * cols_j], r["halo"].at[par, 1], r["hsend"].at[1], r["hrecv"].at[par, 1], left),
        ]
        for c in halo:
            c.start()

        def send(b, k, g):
            at = SLAB * g
            if k == 0:
                return s0[(b + 2) * cols_j + at:(b + 2) * cols_j + at + SLAB, :]
            if k == 1:
                return s0[b * cols_j + at:b * cols_j + at + SLAB, :]
            if k == 2:
                return sup[b * cols_j + at:b * cols_j + at + SLAB, :]
            if k == 3:
                return sdn[b * cols_j + at:b * cols_j + at + SLAB, :]
            sh = quarter if k == 4 else -quarter
            base = (b + 1) * cols_j
            lo, hi = (at + sh) % cols_j, (at + 8 + sh) % cols_j
            return jnp.concatenate([s0[base + lo:base + lo + 8, :], s0[base + hi:base + hi + 8, :]], axis=0)

        def edge_act(i):
            for bb in range(bpc):
                b = order[i * bpc + bb]
                for g in range(cols_j // SLAB):
                    recv = rr[b * cols_j + SLAB * g:b * cols_j + SLAB * g + SLAB, :]
                    for k in range(OFFSETS):
                        o = (bb * OFFSETS + k) * cols_j + SLAB * g
                        hid[i % 2][o:o + SLAB, :] = silu(pre[i % 2][o:o + SLAB, :] + send(b, k, g) + recv).astype(BF16)

        def edge_finish(i):
            y = ys[i % 2]
            for bb in range(bpc):
                b = order[i * bpc + bb]
                for g in range(cols_j // SLAB):
                    total = None
                    for k in range(OFFSETS):
                        o = (bb * OFFSETS + k) * cols_j + SLAB * g
                        eo = i * chunk + o
                        new = (e[eo:eo + SLAB, :].astype(F32) + layer_norm(y[o:o + SLAB, :])).astype(BF16)
                        e[eo:eo + SLAB, :] = new
                        total = new.astype(F32) if total is None else total + new.astype(F32)
                    r["esum"][b * cols_j + SLAB * g:b * cols_j + SLAB * g + SLAB, :] = total.astype(BF16)

        for i in range(nchunk + 2):
            if i < nchunk:
                pre[i % 2][0:chunk, :] = dot(e[i * chunk:(i + 1) * chunk, :], wi[0:latent, :])
            if i == nchunk:
                for c in halo:
                    c.wait()
                low, high = r["halo"][par, 0], r["halo"][par, 1]
                low_w = jnp.concatenate([low[-1:], low[:-1]], axis=0)
                high_w = jnp.concatenate([high[1:], high[:1]], axis=0)
                s0[0:cols_j, :] = jnp.where(me == 0, low_w, low)
                s0[(nblk + 1) * cols_j:, :] = jnp.where(me == n - 1, high_w, high)
            if 1 <= i < nchunk + 1:
                edge_act(i - 1)
                ys[(i - 1) % 2][0:chunk, :] = dot(hid[(i - 1) % 2][0:chunk, :], wo[...])
            if i >= 2:
                edge_finish(i - 2)
        for q in range(2):
            base = q * half
            pre[q][0:half, :] = dot(r["esum"][base:base + half, :], ni[latent:, :])
            act(pre[q], half, hid[q], lambda o, base=base: n1[base + o:base + o + SLAB, :])
            ys[q][0:half, :] = dot(hid[q][0:half, :], no[...])

            def store(o, v, base=base):
                at = slice(base + o, base + o + SLAB)
                h[at, :] = (h[at, :].astype(F32) + v).astype(BF16)

            finish(ys[q], half, store)
        return slot0

    def step_body(s, _):
        x_prev, x_cur = r["xs"].at[s], r["xs"].at[1 - s]
        mean, std, dmean, dstd = (r["ns"][:, i:i + 1] for i in range(4))

        def grid_body(q, _):
            base = pl.multiple_of(q * rows, rows)
            at = pl.ds(base, rows)
            p = pre[0]
            p[0:nvar, :] = (x_prev[:, at] - mean) / std
            p[nvar:2 * nvar, :] = (x_cur[:, at] - mean) / std
            p[2 * nvar:in_feat, :] = r["fs"][s, :, at]
            p[in_feat:, :] = jnp.zeros((p.shape[0] - in_feat, rows), F32)
            hid[0][...] = p[...].astype(BF16)
            pre[1][...] = dot_t(hid[0][...], r["wg"][...])
            act(pre[1], rows, hid[1])
            ys[1][...] = dot(hid[1][...], r["wemb"][0])

            def store(o, v):
                r["gl"][pl.ds(base + o, SLAB), :] = v.astype(BF16)

            finish(ys[1], rows, store)
            pre[0][...] = dot(r["gl"][at, :], r["wi"][0, latent:2 * latent, :])
            act(pre[0], rows, hid[0], lambda o: r["encst"][pl.ds(base + o, SLAB), :])
            ys[0][...] = dot(hid[0][...], r["wo"][0])

            def store_edge(o, v):
                hid[1][o:o + SLAB, :] = (r["g2m"][pl.ds(base + o, SLAB), :].astype(F32) + v).astype(BF16)

            finish(ys[0], rows, store_edge)
            hbase = pl.multiple_of(q * half, half)
            esum = dot(r["ps"][...], hid[1][...]).astype(BF16)
            pre[1][0:half, :] = dot(esum, r["ni"][0, latent:, :])
            act(pre[1], half, hid[0], lambda o: r["nodst"][pl.ds(hbase + o, SLAB), :])
            ys[1][0:half, :] = dot(hid[0][0:half, :], r["no"][0])

            def store_node(o, v):
                r["mcur"][q, o:o + SLAB, :] = (r["mlat"][pl.ds(hbase + o, SLAB), :].astype(F32) + v).astype(BF16)

            finish(ys[1], half, store_node)
            return 0

        lax.fori_loop(0, RATIO, grid_body, 0)
        for off in range(1, n):
            to_blocks(off, lax.rem(me + off, n), me).start()
        r["hin"][pl.ds(2 * me, 2)] = r["mcur"][:, pl.ds(pl.multiple_of(nblk * me, nblk), nblk), :]

        def self_body(q, _):
            base = pl.multiple_of(q * rows, rows)
            at = pl.ds(base, rows)
            pre[0][...] = dot(r["gl"][at, :], r["wself"][0])
            act(pre[0], rows, hid[0])
            ys[0][...] = dot(hid[0][...], r["wself"][1])

            def store(o, v):
                w = pl.ds(base + o, SLAB)
                r["gcur"][w, :] = (r["gl"][w, :].astype(F32) + v).astype(BF16)

            finish(ys[0], rows, store)
            return 0

        lax.fori_loop(0, RATIO, self_body, 0)

        def copy_body(i, _):
            at = pl.ds(pl.multiple_of(i * chunk, chunk), chunk)
            r["e"][at, :] = r["ebase"][at, :]
            return 0

        lax.fori_loop(0, nchunk, copy_body, 0)
        for off in range(1, n):
            to_blocks(off, lax.rem(me + off, n), lax.rem(me + n - off, n)).wait()
        r["h"][...] = dot(r["pfwd"][...], r["hin"][...].reshape(rows, latent)).astype(BF16)

        lax.fori_loop(0, layers, layer_body, s * layers)

        r["yout"][...] = dot(r["pbwd"][...], r["h"][...]).astype(BF16).reshape(cols_j, nblk, latent)
        for off in range(1, n):
            to_grid(off, lax.rem(me + off, n), me).start()
        r["hb"][:, pl.ds(pl.multiple_of(nblk * me, nblk), nblk), :] = r["yout"][pl.ds(2 * me, 2)]
        for off in range(1, n):
            to_grid(off, lax.rem(me + off, n), lax.rem(me + n - off, n)).wait()

        def dec_body(q, _):
            base = pl.multiple_of(q * rows, rows)
            at = pl.ds(base, rows)
            hid[1][...] = dot(r["ex"][...], r["hb"][q]).astype(BF16)
            pre[0][...] = dot(hid[1][...], r["wi"][1, latent:2 * latent, :]) + dot(r["gcur"][at, :], r["wi"][1, 2 * latent:, :])
            act(pre[0], rows, hid[0], lambda o: r["decst"][pl.ds(base + o, SLAB), :])
            ys[0][...] = dot(hid[0][...], r["wo"][1])

            def store_edge(o, v):
                hid[1][o:o + SLAB, :] = (r["m2g"][pl.ds(base + o, SLAB), :].astype(F32) + v).astype(BF16)

            finish(ys[0], rows, store_edge)
            pre[1][...] = dot(r["gcur"][at, :], r["ni"][1, 0:latent, :]) + dot(hid[1][...], r["ni"][1, latent:, :])
            act(pre[1], rows, hid[0])
            ys[1][...] = dot(hid[0][...], r["no"][1])

            def store_node(o, v):
                hid[1][o:o + SLAB, :] = (r["gcur"][pl.ds(base + o, SLAB), :].astype(F32) + v).astype(BF16)

            finish(ys[1], rows, store_node)
            pre[0][...] = dot(hid[1][...], r["woh"][...])
            act(pre[0], rows, hid[0])
            pred = dot_bt(r["wof"][...], hid[0][...])
            x_prev[:, at] = x_cur[:, at] + dstd * pred[0:nvar] + dmean
            return 0

        lax.fori_loop(0, RATIO, dec_body, 0)
        pltpu.make_async_copy(x_prev, r["out"].at[s], r["out_sem"].at[s]).start()
        return 0

    lax.fori_loop(0, 2, step_body, 0)
    for s in range(2):
        pltpu.make_async_copy(r["xs"].at[s], r["out"].at[s], r["out_sem"].at[s]).wait()
    for c in fetch(1, (2 * layers) % 2):
        c.wait()


def solution(mesh):
    n = mesh.shape["gp"]
    row_spec = P(("dp", "gp"))
    edge_spec = P(("dp", "gp"), None, None)
    whole = P()

    def local_run(x_prev, x_cur, forcing, grid_static, g2m_feat, m2g_feat, mesh_feat, mesh_edge_feat, norm_stats, w_grid_in, w_mesh_in, w_eemb_in, w_embed_out, w_edge_in, w_edge_out, w_node_in, w_node_out, w_grid_self, w_out_hidden, w_out_final):
        grid_rows, nvar = x_prev.shape
        rows = mesh_feat.shape[0]
        latent = w_embed_out.shape[-1]
        blocks = w_edge_in.shape[0]
        in_feat = w_grid_in.shape[0]
        shift = rows // 2
        cols_j = n * rows // shift
        nblk = shift // n
        chunk = 2 * OFFSETS * cols_j

        def padded(a, count, axis=0):
            widths = [(0, 0)] * a.ndim
            widths[axis] = (0, count - a.shape[axis])
            return jnp.pad(a, widths)

        fs = jnp.concatenate([forcing.transpose(1, 2, 0), jnp.broadcast_to(grid_static.T[None], (2, grid_static.shape[1], grid_rows))], axis=1)
        gm = jnp.stack([padded(g2m_feat.T.astype(BF16), 16), padded(m2g_feat.T.astype(BF16), 16)])
        edge_t = mesh_edge_feat.transpose(1, 2, 0).reshape(-1, rows).astype(BF16)
        mf = jnp.concatenate([padded(edge_t, 32), padded(mesh_feat.T.astype(BF16), 16)])
        ew = jnp.concatenate([padded(w_mesh_in, 16)[None], padded(w_eemb_in, 16, 1)])
        wof = padded(w_out_final.T, 256)
        inputs = dict(xp_h=x_prev.T, xc_h=x_cur.T, fs_h=fs, ns_h=norm_stats.T, gm_h=gm, mf_h=mf, ew_h=ew, wg_h=w_grid_in, wemb_h=w_embed_out, wei_h=w_edge_in, weo_h=w_edge_out, wni_h=w_node_in, wno_h=w_node_out, wself_h=w_grid_self, woh_h=w_out_hidden, wof_h=wof)
        big = max(rows, chunk)
        vm = pltpu.VMEM
        dma = pltpu.SemaphoreType.DMA
        scratch = dict(
            xs=vm((2, nvar, grid_rows), F32), fs=vm(fs.shape, F32), ns=vm((nvar, 4), F32), gm=vm(gm.shape, BF16), mf=vm(mf.shape, BF16),
            ew=vm(ew.shape, BF16), wg=vm((rows, latent), BF16), wemb=vm(w_embed_out.shape, BF16),
            wi=vm((2, 3 * latent, latent), BF16), wo=vm((2, latent, latent), BF16), ni=vm((2, 2 * latent, latent), BF16), no=vm((2, latent, latent), BF16),
            wself=vm(w_grid_self.shape, BF16), woh=vm(w_out_hidden.shape, BF16), wof=vm(wof.shape, BF16),
            lwi=vm((2, 3 * latent, latent), BF16), lwo=vm((2, latent, latent), BF16), lni=vm((2, 2 * latent, latent), BF16), lno=vm((2, latent, latent), BF16),
            pfwd=vm((rows, rows), BF16), pbwd=vm((rows, rows), BF16), ex=vm((rows, rows // 2), BF16), ps=vm((rows // 2, rows), BF16),
            feat=vm((2, rows // 2, 128), BF16), fin=vm((cols_j, nblk, 128), BF16), featm=vm((rows, 128), BF16), mfp=vm((16, rows), BF16), g2p=vm((16, grid_rows), BF16),
            m2g=vm((grid_rows, latent), BF16), g2m=vm((grid_rows, latent), BF16), mlat=vm((rows, latent), BF16),
            decst=vm((grid_rows, latent), F32), encst=vm((grid_rows, latent), F32), nodst=vm((rows, latent), F32),
            gl=vm((grid_rows, latent), BF16), gcur=vm((grid_rows, latent), BF16), mcur=vm((2, rows // 2, latent), BF16),
            hin=vm((cols_j, nblk, latent), BF16), hb=vm((2, rows // 2, latent), BF16), yout=vm((cols_j, nblk, latent), BF16),
            ebase=vm((OFFSETS * rows, latent), BF16), e=vm((OFFSETS * rows, latent), BF16), h=vm((rows, latent), BF16),
            s0=vm((rows + 2 * cols_j, latent), F32), sup=vm((rows, latent), F32), sdn=vm((rows, latent), F32), rr=vm((rows, latent), F32), n1=vm((rows, latent), F32),
            esum=vm((rows, latent), BF16), halo=vm((2, 2, cols_j, latent), F32),
            p0=vm((big, latent), F32), p1=vm((big, latent), F32), h0=vm((big, latent), BF16), h1=vm((big, latent), BF16), y0=vm((big, latent), F32), y1=vm((big, latent), F32),
            load_sem=dma((20,)), fetch_sem=dma((2, 4)), out_sem=dma((2,)), fsend=dma((n, 2)), frecv=dma((n, 2)), nsend=dma((2,)), nrecv=dma((2,)),
            asend=dma((n,)), arecv=dma((n,)), bsend=dma((n,)), brecv=dma((n,)), hsend=dma((2,)), hrecv=dma((2, 2)),
        )
        cfg = dict(names=(*inputs, "out", *scratch), n=n, rows=rows, latent=latent, shift=shift, layers=blocks - 2, nvar=nvar, in_feat=in_feat)
        anywhere = pl.BlockSpec(memory_space=pl.ANY)
        out = pl.pallas_call(
            functools.partial(kernel, cfg),
            out_shape=jax.ShapeDtypeStruct((2, nvar, grid_rows), F32),
            in_specs=[anywhere] * len(inputs),
            out_specs=anywhere,
            scratch_shapes=list(scratch.values()),
            compiler_params=pltpu.CompilerParams(collective_id=0, has_side_effects=True, vmem_limit_bytes=66_000_000),
        )(*inputs.values())
        return out[0].T, out[1].T

    in_specs = (row_spec, row_spec, edge_spec, row_spec, row_spec, row_spec, row_spec, edge_spec, whole) + (whole,) * 11
    return jax.shard_map(local_run, mesh=mesh, in_specs=in_specs, out_specs=(row_spec, row_spec), check_vma=False)
```

```python
import functools
import types

import jax
import jax.numpy as jnp
from jax import lax
from jax.experimental import pallas as pl
from jax.experimental.pallas import tpu as pltpu
from jax.sharding import PartitionSpec as P

F32 = jnp.float32
BF16 = jnp.bfloat16
SLAB = 16
RATIO = 2
OFFSETS = 6
LOWER = ("E6", "A7", "S7", "F0", "F1", "A0", "nf1", "E7", "na1", "nf2", "na2", "A1", "ns2", "S0", "F3", "F2", "ne2", "ns1", "ne1", "S1", "E0", "A2", "E1", "S2", "ps2")
UPPER = ("ro2", "ps1", "E2", "ro1", "pr1", "A3", "S3", "pr2", "F4", "A4", "E3", "F5", "S4", "nf0", "A5", "F6", "na0", "S5", "ns0", "E4", "A6", "ne0", "KEEP", "E5", "S6", "F7", "ps0", "ro0", "pr0")


def dot(a, b):
    return jnp.dot(a, b, preferred_element_type=F32)


def dot_t(a, b):
    return lax.dot_general(a, b, (((0,), (0,)), ((), ())), preferred_element_type=F32)


def dot_bt(a, b):
    return lax.dot_general(a, b, (((1,), (1,)), ((), ())), preferred_element_type=F32)


def silu(x):
    return x * lax.logistic(x)


def layer_norm(y):
    centred = y - jnp.mean(y, axis=-1, keepdims=True)
    spread = jnp.mean(centred * centred, axis=-1, keepdims=True)
    return centred * lax.rsqrt(spread + 1e-5)


def kernel(cfg, *refs):
    r = types.SimpleNamespace(**dict(zip(cfg.names, refs, strict=True)))
    n, rows, latent, shift, layers = cfg.n, cfg.rows, cfg.latent, cfg.shift, cfg.layers
    nvar, in_feat = cfg.nvar, cfg.in_feat
    cols_j = n * rows // shift
    nblk = shift // n
    quarter = cols_j // 4
    grid_rows = RATIO * rows
    per_blk = OFFSETS * cols_j
    bpc = 2
    chunk = bpc * per_blk
    nchunk = nblk // bpc
    pair = nblk // 2
    chunks = [(2 * i + 1, 2 * i + 2) for i in range(pair // 2 - 1)] + [(0, pair - 1)] + [(pair + 2 * i, pair + 2 * i + 1) for i in range(pair // 2)]
    flat = [p for c in chunks for p in c]
    me = lax.axis_index("gp")
    left = lax.rem(me + n - 1, n)
    right = lax.rem(me + 1, n)
    pre, hid, ys = (r.p0, r.p1), (r.h0, r.h1), (r.y0, r.y1)

    def remote(src, dst, send, recv, dev):
        return pltpu.make_async_remote_copy(src_ref=src, dst_ref=dst, send_sem=send, recv_sem=recv, device_id={"gp": dev}, device_id_type=pl.DeviceIdType.MESH)

    last = layers + 1
    pairs = dict(
        mfr=(r.mf_h, r.mfr), mer=(r.me_h, r.mer), g2r=(r.g2_h, r.g2r), m2r=(r.m2_h, r.m2r), gsr=(r.gs_h, r.gsr), frr=(r.fr_h, r.frr), nsr=(r.ns_h, r.nsr),
        wmr=(r.wm_h, r.wmr), wer=(r.we_h, r.wer), xp=(r.xp_h, r.xs.at[0]), xc=(r.xc_h, r.xs.at[1]), wg=(r.wg_h, r.wg.at[0:in_feat]), wemb=(r.wemb_h, r.wemb),
        wi1=(r.wei_h.at[last], r.wi.at[1]), wi0=(r.wei_h.at[0], r.wi.at[0]), ni0=(r.wni_h.at[0], r.ni.at[0]), wo0=(r.weo_h.at[0], r.wo.at[0]), no0=(r.wno_h.at[0], r.no.at[0]),
        wself=(r.wself_h, r.wself), wo1=(r.weo_h.at[last], r.wo.at[1]), ni1=(r.wni_h.at[last], r.ni.at[1]), no1=(r.wno_h.at[last], r.no.at[1]), woh=(r.woh_h, r.woh), wof=(r.wof_h, r.wof),
    )
    load = types.SimpleNamespace(**{key: pltpu.make_async_copy(src, dst, r.load_sem.at[i]) for i, (key, (src, dst)) in enumerate(pairs.items())})

    def fetch(layer, slot):
        pairs = ((r.wei_h, r.lwi), (r.weo_h, r.lwo), (r.wni_h, r.lni), (r.wno_h, r.lno))
        return [pltpu.make_async_copy(src.at[layer], dst.at[slot], r.fetch_sem.at[slot, i]) for i, (src, dst) in enumerate(pairs)]

    for c in vars(load).values():
        c.start()
    for c in fetch(1, 0):
        c.start()

    barrier = pltpu.get_barrier_semaphore()
    for off in range(1, n):
        pl.semaphore_signal(barrier, inc=1, device_id={"gp": lax.rem(me + off, n)}, device_id_type=pl.DeviceIdType.MESH)

    def iota(shape, dim):
        return lax.broadcasted_iota(jnp.int32, shape, dim)

    def onehot(pred):
        return jnp.where(pred, 1.0, 0.0).astype(BF16)

    def slot_of(row):
        jp = lax.rem(lax.rem(row, cols_j) + (cols_j - 1), cols_j)
        return jp * nblk + lax.rem(lax.div(row, cols_j) + 1, nblk)

    for t in range(rows // 128):
        sl = slice(128 * t, 128 * t + 128)
        r.pfwd[sl, :] = onehot(iota((128, rows), 1) == slot_of(iota((128, rows), 0) + 128 * t))
        r.pbwd[sl, :] = onehot(iota((128, rows), 0) + 128 * t == slot_of(iota((128, rows), 1)))
    half = rows // 2
    r.ex[...] = onehot(lax.div(iota((rows, half), 0), RATIO) == iota((rows, half), 1))
    r.ps[...] = onehot(iota((half, rows), 0) == lax.div(iota((half, rows), 1), RATIO))
    for ref in (r.s0, r.sup, r.sdn, r.rr, r.n1, r.edge_s, r.keep, r.esum):
        ref[...] = jnp.zeros(ref.shape, ref.dtype)
    r.wg[in_feat:, :] = jnp.zeros((r.wg.shape[0] - in_feat, latent), BF16)

    def act(p, count, hidden, add=None):
        for o in range(0, count, SLAB):
            x = p[o:o + SLAB, :]
            if add is not None:
                x = x + add(o)
            hidden[o:o + SLAB, :] = silu(x).astype(BF16)

    def finish(y, count, store):
        for o in range(0, count, SLAB):
            store(o, layer_norm(y[o:o + SLAB, :]))

    st = r.p0
    wide = grid_rows // latent

    def staged(value, count=16):
        st[0:count, :] = jnp.zeros((count, latent), F32)
        st[0:value.shape[0], :] = value.astype(F32)
        return st[0:count, :].astype(BF16)

    for c in (load.mfr, load.mer, load.g2r, load.m2r, load.gsr, load.frr, load.nsr, load.wmr, load.wer):
        c.wait()
    r.ew[0] = staged(r.wmr[...])
    for i in range(3):
        r.ew[i + 1] = staged(r.wer[i])
    for i in range(wide):
        at = slice(i * latent, (i + 1) * latent)
        r.gm[0, :, at] = staged(r.g2r[:, at])
        r.gm[1, :, at] = staged(r.m2r[:, at])
    r.mf[32:48, :] = staged(r.mfr[...])
    st[0:32, :] = jnp.zeros((32, latent), F32)
    for k in range(OFFSETS):
        st[4 * k:4 * k + 4, :] = r.mer[k]
    r.mf[0:32, :] = st[0:32, :].astype(BF16)
    force = r.frr.shape[0]
    for i in range(2):
        r.fs[i, 0:force, :] = r.frr[:, i, :]
        r.fs[i, force:force + r.gsr.shape[0], :] = r.gsr[...]
    st[0:128, :] = jnp.zeros((128, latent), F32)
    st[0:4, 0:nvar] = r.nsr[...]
    r.ns[...] = jnp.transpose(st[0:128, 0:256])
    eye = onehot(iota((32, 128), 0) == iota((32, 128), 1))
    r.feat[...] = dot_t(r.mf[0:32, :], eye).astype(BF16).reshape(2, half, 128)
    def grid_embed(s, base):
        at = pl.ds(base, rows)
        mean, std = (r.ns[0:nvar, i:i + 1] for i in (0, 1))
        p = r.p0
        p[0:nvar, :] = (r.xs[s, :, at] - mean) / std
        p[nvar:2 * nvar, :] = (r.xs[1 - s, :, at] - mean) / std
        p[2 * nvar:in_feat, :] = r.fs[s, 0:in_feat - 2 * nvar, at]
        p[in_feat:, :] = jnp.zeros((p.shape[0] - in_feat, rows), F32)
        r.h0[...] = p[...].astype(BF16)
        r.p1[...] = dot_t(r.h0[...], r.wg[...])
        act(r.p1, rows, r.h1)
        r.y1[...] = dot(r.h1[...], r.wemb[0])

        def store(o, v):
            r.gl[pl.ds(base + o, SLAB), :] = v.astype(BF16)

        finish(r.y1, rows, store)

    def first_embed(q, _):
        grid_embed(0, pl.multiple_of(q * rows, rows))
        return 0

    for c in (load.xp, load.xc, load.wg, load.wemb):
        c.wait()
    lax.fori_loop(0, RATIO, first_embed, 0)
    pl.semaphore_wait(barrier, n - 1)

    def feat_copy(off, jj, dev, owner):
        slot = lax.rem(2 * owner + jj + cols_j - 1, cols_j)
        return remote(r.feat.at[jj, pl.ds(pl.multiple_of(nblk * dev, nblk), nblk), :], r.fin.at[slot], r.fsend.at[off, jj], r.frecv.at[off, jj], dev)

    nb_copies = [
        remote(r.mf.at[32:48, 0:half], r.mfp.at[:, half:], r.nsend.at[0], r.nrecv.at[0], left),
        remote(r.gm.at[0, :, 0:rows], r.g2p.at[:, rows:], r.nsend.at[1], r.nrecv.at[1], left),
    ]
    for c in nb_copies:
        c.start()
    for off in range(1, n):
        for jj in range(2):
            feat_copy(off, jj, lax.rem(me + off, n), me).start()
    for jj in range(2):
        r.fin[lax.rem(2 * me + jj + cols_j - 1, cols_j)] = r.feat[jj, pl.ds(pl.multiple_of(nblk * me, nblk), nblk), :]
    r.mfp[:, 0:half] = r.mf[32:48, half:]
    r.g2p[:, 0:rows] = r.gm[0, :, rows:]


    def embed(lhs_t, w_first, w_second, store):
        r.p0[0:rows, :] = dot_t(lhs_t, w_first)
        act(r.p0, rows, r.h0)
        r.y0[0:rows, :] = dot(r.h0[0:rows, :], w_second)
        finish(r.y0, rows, store)

    load.wi1.wait()

    def m2g_body(q, _):
        base = pl.multiple_of(q * rows, rows)

        def store(o, v):
            r.m2g[pl.ds(base + o, SLAB), :] = v.astype(BF16)

        embed(r.gm[1, :, pl.ds(base, rows)], r.ew[2], r.wemb[3], store)
        r.decst[pl.ds(base, rows), :] = dot(r.m2g[pl.ds(base, rows), :], r.wi[1, 0:latent, :])
        return 0

    lax.fori_loop(0, RATIO, m2g_body, 0)

    for c in nb_copies:
        c.wait()
    load.wi0.wait()
    load.ni0.wait()

    def store_mesh(o, v):
        r.mlat[o:o + SLAB, :] = v.astype(BF16)

    embed(r.mfp[...], r.ew[0], r.wemb[1], store_mesh)
    r.nodst[...] = dot(r.mlat[...], r.ni[0, 0:latent, :])

    def g2m_body(q, _):
        base = pl.multiple_of(q * rows, rows)
        hbase = pl.multiple_of(q * half, half)

        def store(o, v):
            r.g2m[pl.ds(base + o, SLAB), :] = v.astype(BF16)

        embed(r.g2p[:, pl.ds(base, rows)], r.ew[1], r.wemb[2], store)
        r.h1[0:rows, :] = dot(r.ex[...], r.mlat[pl.ds(hbase, half), :]).astype(BF16)
        r.encst[pl.ds(base, rows), :] = dot(r.g2m[pl.ds(base, rows), :], r.wi[0, 0:latent, :]) + dot(r.h1[0:rows, :], r.wi[0, 2 * latent:, :])
        return 0

    lax.fori_loop(0, RATIO, g2m_body, 0)

    for c in (load.wo0, load.no0, load.wself):
        c.wait()

    def late_static():
        for c in (load.wo1, load.ni1, load.no1, load.woh, load.wof):
            c.wait()
        for off in range(1, n):
            for jj in range(2):
                feat_copy(off, jj, lax.rem(me + off, n), lax.rem(me + n - off, n)).wait()
        r.featm[...] = dot(r.pfwd[...], r.fin[...].reshape(rows, 128)).astype(BF16)

        def edge_body(k, _):
            sel = onehot(iota((128, 16), 0) == iota((128, 16), 1) + 4 * k)
            sel = jnp.where(iota((128, 16), 1) < 4, sel, jnp.zeros_like(sel))
            w_k = dot(sel, r.ew[3]).astype(BF16)
            r.p0[0:rows, :] = dot(r.featm[...], w_k)
            act(r.p0, rows, r.h0)
            r.y0[0:rows, :] = dot(r.h0[0:rows, :], r.wemb[4])

            def store(o, v):
                pos = flat.index(o // cols_j)
                at = pl.multiple_of(pos * per_blk + (o % cols_j // SLAB * OFFSETS + k) * SLAB, SLAB)
                r.ebase[pl.ds(at, SLAB), :] = v.astype(BF16)

            finish(r.y0, rows, store)
            return 0

        lax.fori_loop(0, OFFSETS, edge_body, 0)

    far_first = sorted(range(1, n), key=lambda off: -min(off, n - off))

    def to_blocks(off, q, dev, owner):
        return remote(r.mcur.at[q, pl.ds(pl.multiple_of(nblk * dev, nblk), nblk), :], r.hin.at[2 * owner + q], r.asend.at[off, q], r.arecv.at[off, q], dev)

    def to_grid(off, q, dev, owner):
        return remote(r.yout.at[2 * dev + q], r.hb.at[q, pl.ds(pl.multiple_of(nblk * owner, nblk), nblk), :], r.bsend.at[off, q], r.brecv.at[off, q], dev)

    s0, sup, sdn, rr, n1, e, h, esum = r.s0, r.sup, r.sdn, r.rr, r.n1, r.e, r.h, r.esum
    npre, nhid, nys = r.np, r.nh, r.ny
    group = rows // 2

    def halo_copies(par):
        lo, hi = (nblk - 2) * cols_j, (nblk - 1) * cols_j
        return [
            remote(s0.at[lo:lo + cols_j], r.halo.at[par, 0], r.hsend.at[0], r.hrecv.at[par, 0], right),
            remote(s0.at[hi:hi + cols_j], r.halo.at[par, 1], r.hsend.at[1], r.hrecv.at[par, 1], left),
        ]

    def take_halo(par):
        for c in halo_copies(par):
            c.wait()
        low, high = r.halo[par, 0], r.halo[par, 1]
        low_w = jnp.concatenate([low[-1:], low[:-1]], axis=0)
        high_w = jnp.concatenate([high[1:], high[:1]], axis=0)
        r.edge_s[0] = jnp.where(me == 0, low_w, low)
        r.edge_s[1] = jnp.where(me == n - 1, high_w, high)

    def send(p, k, g):
        at = slice(SLAB * g, SLAB * g + SLAB)
        if k == 0:
            if p == nblk - 2:
                return r.edge_s[1, at, :]
            if p == nblk - 1:
                return r.keep[at, :]
            base = (p + 1) % nblk * cols_j
            return s0[base + SLAB * g:base + SLAB * g + SLAB, :]
        if k == 1:
            if p == nblk - 1:
                return r.edge_s[0, at, :]
            base = (p - 1) % nblk * cols_j
            return s0[base + SLAB * g:base + SLAB * g + SLAB, :]
        base = p * cols_j
        if k in (2, 3):
            return (sup, sdn)[k - 2][base + SLAB * g:base + SLAB * g + SLAB, :]
        sh = quarter if k == 4 else -quarter
        lo, hi = (SLAB * g + sh) % cols_j, (SLAB * g + 8 + sh) % cols_j
        return jnp.concatenate([s0[base + lo:base + lo + 8, :], s0[base + hi:base + hi + 8, :]], axis=0)

    def edge_act(i):
        for bb, p in enumerate(chunks[i]):
            for g in range(cols_j // SLAB):
                recv = rr[p * cols_j + SLAB * g:p * cols_j + SLAB * g + SLAB, :]
                for k in range(OFFSETS):
                    o = bb * per_blk + (g * OFFSETS + k) * SLAB
                    hid[i % 2][o:o + SLAB, :] = silu(pre[i % 2][o:o + SLAB, :] + send(p, k, g) + recv).astype(BF16)

    def edge_finish(i):
        rows6 = OFFSETS * SLAB
        for bb, p in enumerate(chunks[i]):
            for g in range(cols_j // SLAB):
                o = bb * per_blk + g * rows6
                eo = i * chunk + o
                new = (e[eo:eo + rows6, :].astype(F32) + layer_norm(ys[i % 2][o:o + rows6, :])).astype(BF16)
                e[eo:eo + rows6, :] = new
                total = new[0:SLAB].astype(F32)
                for k in range(1, OFFSETS):
                    total = total + new[k * SLAB:(k + 1) * SLAB].astype(F32)
                esum[p * cols_j + SLAB * g:p * cols_j + SLAB * g + SLAB, :] = total.astype(BF16)

    def edge_first(i, wi):
        pre[i % 2][0:chunk, :] = dot(e[i * chunk:(i + 1) * chunk, :], wi[0:latent, :])

    def edge_second(i, wo):
        ys[i % 2][0:chunk, :] = dot(hid[i % 2][0:chunk, :], wo[...])

    groups = ((0, group), (group, group // 2), (group + group // 2, group // 2))

    def project_send(g, wi):
        o, count = groups[g]
        s0[o:o + count, :] = dot(h[o:o + count, :], wi[latent:2 * latent, :])

    def roll_send(g):
        o, count = groups[g]
        for at in range(o, o + count, cols_j):
            blk = s0[at:at + cols_j, :]
            sup[at:at + cols_j, :] = jnp.concatenate([blk[1:], blk[:1]], axis=0)
            sdn[at:at + cols_j, :] = jnp.concatenate([blk[-1:], blk[:-1]], axis=0)

    def project_rest(g, wi, ni):
        o, count = groups[g]
        rr[o:o + count, :] = dot(h[o:o + count, :], wi[2 * latent:, :])
        n1[o:o + count, :] = dot(h[o:o + count, :], ni[0:latent, :])

    def node_first(g, ni):
        o, count = groups[g]
        npre[o:o + count, :] = dot(esum[o:o + count, :], ni[latent:, :])

    def node_act(g):
        o, count = groups[g]
        for at in range(o, o + count, SLAB):
            nhid[at:at + SLAB, :] = silu(npre[at:at + SLAB, :] + n1[at:at + SLAB, :]).astype(BF16)

    def node_second(g, no):
        o, count = groups[g]
        nys[o:o + count, :] = dot(nhid[o:o + count, :], no[...])

    def node_finish(g):
        o, count = groups[g]
        step = 4 * SLAB
        for at in range(o, o + count, step):
            h[at:at + step, :] = (h[at:at + step, :].astype(F32) + layer_norm(nys[at:at + step, :])).astype(BF16)

    def weights(i):
        return [x.at[i] for x in (r.lwi, r.lwo, r.lni, r.lno)]

    def layer_body(t, first):
        cur, was, nxt = (lax.rem(first + t + i, 3) for i in (0, 2, 1))
        par = lax.rem(first + t, 2)
        wi, wo, ni, no = weights(cur)
        wi_n, _, ni_n, _ = weights(nxt)
        _, wo_w, ni_w, no_w = weights(was)

        @pl.when(t > 0)
        def _():
            take_halo(1 - par)

        def run(stages, table):
            for stage in stages:
                name = stage.rstrip("0123456789")
                table[name](*(int(d) for d in stage[len(name):]))

        last_chunk = nchunk - 1
        run(LOWER, dict(
            A=edge_act, E=edge_finish, F=lambda i: edge_first(i, wi), S=lambda i: edge_second(i, wo_w if i == last_chunk else wo),
            nf=lambda g: node_first(g, ni_w), na=node_act, ns=lambda g: node_second(g, no_w), ne=node_finish,
            ps=lambda g: project_send(g, wi), ro=roll_send))
        for c in halo_copies(par):
            c.start()
        for c in fetch(jnp.where(t + 1 < layers, t + 2, 1), nxt):
            c.wait()
        for c in fetch(jnp.where(t + 2 < layers, t + 3, t + 3 - layers), was):
            c.start()

        def keep():
            r.keep[...] = s0[0:cols_j, :]

        run(UPPER, dict(
            A=edge_act, E=edge_finish, F=lambda i: edge_first(i, wi), S=lambda i: edge_second(i, wo),
            nf=lambda g: node_first(g, ni), na=node_act, ns=lambda g: node_second(g, no), ne=node_finish,
            ps=lambda g: project_send(g, wi if g else wi_n), pr=lambda g: project_rest(g, wi if g else wi_n, ni if g else ni_n), ro=roll_send, KEEP=keep))
        return first

    def run_layers(first):
        was, cur = (lax.rem(first + i, 3) for i in (2, 0))
        wi, _, ni, _ = weights(cur)
        r.lwo[was] = jnp.zeros((latent, latent), BF16)
        r.lno[was] = jnp.zeros((latent, latent), BF16)
        r.lni[was, latent:, :] = jnp.zeros((latent, latent), BF16)
        r.y0[...] = jnp.zeros(r.y0.shape, F32)
        project_send(0, wi)
        roll_send(0)
        project_rest(0, wi, ni)
        lax.fori_loop(0, layers, layer_body, first)
        was = lax.rem(first + layers + 2, 3)
        take_halo(lax.rem(first + layers + 1, 2))
        edge_act(7)
        edge_second(7, r.lwo.at[was])
        edge_finish(6)
        edge_finish(7)
        for g in (1, 2):
            node_first(g, r.lni.at[was])
            node_act(g)
            node_second(g, r.lno.at[was])
            node_finish(g)

    def step_body(s, _):
        x_prev, x_cur = r.xs.at[s], r.xs.at[1 - s]
        dmean, dstd = (r.ns[0:nvar, i:i + 1] for i in (2, 3))

        def grid_body(q, _):
            base = pl.multiple_of(q * rows, rows)
            at = pl.ds(base, rows)

            @pl.when(s > 0)
            def _():
                grid_embed(s, base)

            r.p0[...] = dot(r.gl[at, :], r.wi[0, latent:2 * latent, :])
            act(r.p0, rows, r.h0, lambda o: r.encst[pl.ds(base + o, SLAB), :])
            r.y0[...] = dot(r.h0[...], r.wo[0])

            def store_edge(o, v):
                r.h1[o:o + SLAB, :] = (r.g2m[pl.ds(base + o, SLAB), :].astype(F32) + v).astype(BF16)

            finish(r.y0, rows, store_edge)
            hbase = pl.multiple_of(q * half, half)
            esum = dot(r.ps[...], r.h1[...]).astype(BF16)
            r.p1[0:half, :] = dot(esum, r.ni[0, latent:, :])
            act(r.p1, half, r.h0, lambda o: r.nodst[pl.ds(hbase + o, SLAB), :])
            r.y1[0:half, :] = dot(r.h0[0:half, :], r.no[0])

            def store_node(o, v):
                r.mcur[q, o:o + SLAB, :] = (r.mlat[pl.ds(hbase + o, SLAB), :].astype(F32) + v).astype(BF16)

            finish(r.y1, half, store_node)
            for off in far_first:
                to_blocks(off, q, lax.rem(me + off, n), me).start()
            r.hin[2 * me + q] = r.mcur[q, pl.ds(pl.multiple_of(nblk * me, nblk), nblk), :]
            return 0

        lax.fori_loop(0, RATIO, grid_body, 0)
        def self_body(q, _):
            base = pl.multiple_of(q * rows, rows)
            at = pl.ds(base, rows)
            r.p0[...] = dot(r.gl[at, :], r.wself[0])
            act(r.p0, rows, r.h0)
            r.y0[...] = dot(r.h0[...], r.wself[1])

            def store(o, v):
                w = pl.ds(base + o, SLAB)
                r.gcur[w, :] = (r.gl[w, :].astype(F32) + v).astype(BF16)

            finish(r.y0, rows, store)
            return 0

        lax.fori_loop(0, RATIO, self_body, 0)
        pl.when(s == 0)(late_static)

        def copy_body(i, _):
            at = pl.ds(pl.multiple_of(i * chunk, chunk), chunk)
            r.e[at, :] = r.ebase[at, :]
            return 0

        lax.fori_loop(0, nchunk, copy_body, 0)
        for q in range(2):
            for off in far_first:
                to_blocks(off, q, lax.rem(me + off, n), lax.rem(me + n - off, n)).wait()
        r.h[...] = dot(r.pfwd[...], r.hin[...].reshape(rows, latent)).astype(BF16)

        run_layers(s * layers)

        r.yout[...] = dot(r.pbwd[...], r.h[...]).astype(BF16).reshape(cols_j, nblk, latent)
        for q in range(2):
            for off in far_first:
                to_grid(off, q, lax.rem(me + off, n), me).start()
        for q in range(2):
            r.hb[q, pl.ds(pl.multiple_of(nblk * me, nblk), nblk), :] = r.yout[2 * me + q]

        def dec_body(q, _):
            base = pl.multiple_of(q * rows, rows)
            at = pl.ds(base, rows)
            for off in far_first:
                to_grid(off, q, lax.rem(me + off, n), lax.rem(me + n - off, n)).wait()
            r.h1[...] = dot(r.ex[...], r.hb[q]).astype(BF16)
            r.p0[...] = dot(r.h1[...], r.wi[1, latent:2 * latent, :]) + dot(r.gcur[at, :], r.wi[1, 2 * latent:, :])
            act(r.p0, rows, r.h0, lambda o: r.decst[pl.ds(base + o, SLAB), :])
            r.y0[...] = dot(r.h0[...], r.wo[1])

            def store_edge(o, v):
                r.h1[o:o + SLAB, :] = (r.m2g[pl.ds(base + o, SLAB), :].astype(F32) + v).astype(BF16)

            finish(r.y0, rows, store_edge)
            r.p1[...] = dot(r.gcur[at, :], r.ni[1, 0:latent, :]) + dot(r.h1[...], r.ni[1, latent:, :])
            act(r.p1, rows, r.h0)
            r.y1[...] = dot(r.h0[...], r.no[1])

            def store_node(o, v):
                r.h1[o:o + SLAB, :] = (r.gcur[pl.ds(base + o, SLAB), :].astype(F32) + v).astype(BF16)

            finish(r.y1, rows, store_node)
            r.p0[...] = dot(r.h1[...], r.woh[...])
            act(r.p0, rows, r.h0)
            pred = dot_bt(r.wof[...], r.h0[...])
            x_prev[:, at] = x_cur[:, at] + dstd * pred + dmean
            return 0

        lax.fori_loop(0, RATIO, dec_body, 0)
        pltpu.make_async_copy(x_prev, r.out.at[s], r.out_sem.at[s]).start()
        return 0

    for c in fetch(1, 0):
        c.wait()
    for c in fetch(2, 1):
        c.start()
    lax.fori_loop(0, 2, step_body, 0)
    for s in range(2):
        pltpu.make_async_copy(r.xs.at[s], r.out.at[s], r.out_sem.at[s]).wait()
    for c in fetch(1, (2 * layers + 1) % 3):
        c.wait()


def solution(mesh):
    n = mesh.shape["gp"]
    row_spec = P(("dp", "gp"))
    edge_spec = P(("dp", "gp"), None, None)
    whole = P()

    def local_run(x_prev, x_cur, forcing, grid_static, g2m_feat, m2g_feat, mesh_feat, mesh_edge_feat, norm_stats, w_grid_in, w_mesh_in, w_eemb_in, w_embed_out, w_edge_in, w_edge_out, w_node_in, w_node_out, w_grid_self, w_out_hidden, w_out_final):
        grid_rows, nvar = x_prev.shape
        rows = mesh_feat.shape[0]
        latent = w_embed_out.shape[-1]
        blocks = w_edge_in.shape[0]
        in_feat = w_grid_in.shape[0]
        shift = rows // 2
        cols_j = n * rows // shift
        nblk = shift // n
        chunk = 2 * OFFSETS * cols_j

        inputs = dict(xp_h=x_prev.T, xc_h=x_cur.T, fr_h=forcing.transpose(2, 1, 0), gs_h=grid_static.T, g2_h=g2m_feat.T, m2_h=m2g_feat.T, mf_h=mesh_feat.T, me_h=mesh_edge_feat.transpose(1, 2, 0), ns_h=norm_stats, wm_h=w_mesh_in, we_h=w_eemb_in, wg_h=w_grid_in, wemb_h=w_embed_out, wei_h=w_edge_in, weo_h=w_edge_out, wni_h=w_node_in, wno_h=w_node_out, wself_h=w_grid_self, woh_h=w_out_hidden, wof_h=w_out_final.T)
        big = max(rows, chunk)
        vm = pltpu.VMEM
        dma = pltpu.SemaphoreType.DMA
        scratch = dict(
            xs=vm((2, nvar, grid_rows), F32), fs=vm((2, 16, grid_rows), F32), ns=vm((256, 128), F32), gm=vm((2, 16, grid_rows), BF16), mf=vm((48, rows), BF16),
            ew=vm((4, 16, latent), BF16), wg=vm((rows, latent), BF16), wemb=vm(w_embed_out.shape, BF16),
            wi=vm((2, 3 * latent, latent), BF16), wo=vm((2, latent, latent), BF16), ni=vm((2, 2 * latent, latent), BF16), no=vm((2, latent, latent), BF16),
            wself=vm(w_grid_self.shape, BF16), woh=vm(w_out_hidden.shape, BF16),
            lwi=vm((3, 3 * latent, latent), BF16), lwo=vm((3, latent, latent), BF16), lni=vm((3, 2 * latent, latent), BF16), lno=vm((3, latent, latent), BF16),
            pfwd=vm((rows, rows), BF16), pbwd=vm((rows, rows), BF16), ex=vm((rows, rows // 2), BF16), ps=vm((rows // 2, rows), BF16),
            feat=vm((2, rows // 2, 128), BF16), fin=vm((cols_j, nblk, 128), BF16), featm=vm((rows, 128), BF16), mfp=vm((16, rows), BF16), g2p=vm((16, grid_rows), BF16),
            m2g=vm((grid_rows, latent), BF16), g2m=vm((grid_rows, latent), BF16), mlat=vm((rows, latent), BF16),
            decst=vm((grid_rows, latent), F32), encst=vm((grid_rows, latent), F32), nodst=vm((rows, latent), F32),
            gl=vm((grid_rows, latent), BF16), gcur=vm((grid_rows, latent), BF16), mcur=vm((2, rows // 2, latent), BF16),
            hin=vm((cols_j, nblk, latent), BF16), hb=vm((2, rows // 2, latent), BF16), yout=vm((cols_j, nblk, latent), BF16),
            ebase=vm((OFFSETS * rows, latent), BF16), e=vm((OFFSETS * rows, latent), BF16), h=vm((rows, latent), BF16),
            s0=vm((rows, latent), F32), sup=vm((rows, latent), F32), sdn=vm((rows, latent), F32), rr=vm((rows, latent), F32), n1=vm((rows, latent), F32),
            esum=vm((rows, latent), BF16), edge_s=vm((2, cols_j, latent), F32), keep=vm((cols_j, latent), F32), np=vm((rows, latent), F32), nh=vm((rows, latent), BF16), ny=vm((rows, latent), F32), halo=vm((2, 2, cols_j, latent), F32),
            p0=vm((big, latent), F32), p1=vm((big, latent), F32), h0=vm((big, latent), BF16), h1=vm((big, latent), BF16), y0=vm((big, latent), F32), y1=vm((big, latent), F32),
            wof=vm((nvar, latent), BF16), mfr=vm((mesh_feat.shape[1], rows), F32), mer=vm((*mesh_edge_feat.shape[1:], rows), F32), g2r=vm((g2m_feat.shape[1], grid_rows), F32), m2r=vm((m2g_feat.shape[1], grid_rows), F32),
            gsr=vm((grid_static.shape[1], grid_rows), F32), frr=vm((forcing.shape[2], forcing.shape[1], grid_rows), F32), nsr=vm(norm_stats.shape, F32), wmr=vm(w_mesh_in.shape, BF16), wer=vm(w_eemb_in.shape, BF16),
            load_sem=dma((24,)), fetch_sem=dma((3, 4)), out_sem=dma((2,)), fsend=dma((n, 2)), frecv=dma((n, 2)), nsend=dma((2,)), nrecv=dma((2,)),
            asend=dma((n, 2)), arecv=dma((n, 2)), bsend=dma((n, 2)), brecv=dma((n, 2)), hsend=dma((2,)), hrecv=dma((2, 2)),
        )
        cfg = types.SimpleNamespace(names=(*inputs, "out", *scratch), n=n, rows=rows, latent=latent, shift=shift, layers=blocks - 2, nvar=nvar, in_feat=in_feat)
        anywhere = pl.BlockSpec(memory_space=pl.ANY)
        out = pl.pallas_call(
            functools.partial(kernel, cfg),
            out_shape=jax.ShapeDtypeStruct((2, nvar, grid_rows), F32),
            in_specs=[anywhere] * len(inputs),
            out_specs=anywhere,
            scratch_shapes=list(scratch.values()),
            compiler_params=pltpu.CompilerParams(collective_id=0, has_side_effects=True, vmem_limit_bytes=66_000_000),
        )(*inputs.values())
        return out[0].T, out[1].T

    in_specs = (row_spec, row_spec, edge_spec, row_spec, row_spec, row_spec, row_spec, edge_spec, whole) + (whole,) * 11
    return jax.shard_map(local_run, mesh=mesh, in_specs=in_specs, out_specs=(row_spec, row_spec), check_vma=False)
```

```python
import functools
import types

import jax
import jax.numpy as jnp
from jax import lax
from jax.experimental import pallas as pl
from jax.experimental.pallas import tpu as pltpu
from jax.sharding import PartitionSpec as P

F32 = jnp.float32
BF16 = jnp.bfloat16
SLAB = 16
RATIO = 2
OFFSETS = 6
LOWER = ("E6", "A7", "S7", "F0", "F1", "A0", "nf1", "E7", "na1", "nf2", "na2", "A1", "ns2", "S0", "F3", "E0", "ne2", "ns1", "F2", "ne1", "S1", "A2", "E1", "S2", "ps2")
UPPER = ("ro2", "ps1", "E2", "ro1", "pr1", "A3", "S3", "pr2", "F4", "A4", "E3", "F5", "F6", "S4", "nf0", "A5", "na0", "S5", "ns0", "E4", "A6", "ne0", "KEEP", "S6", "E5", "F7", "ps0", "ro0", "pr0")


def dot(a, b):
    return jnp.dot(a, b, preferred_element_type=F32)


def dot_t(a, b):
    return lax.dot_general(a, b, (((0,), (0,)), ((), ())), preferred_element_type=F32)


def dot_bt(a, b):
    return lax.dot_general(a, b, (((1,), (1,)), ((), ())), preferred_element_type=F32)


def silu(x):
    return x * lax.logistic(x)


def layer_norm(y):
    centred = y - jnp.mean(y, axis=-1, keepdims=True)
    spread = jnp.mean(centred * centred, axis=-1, keepdims=True)
    return centred * lax.rsqrt(spread + 1e-5)


def kernel(cfg, *refs):
    r = types.SimpleNamespace(**dict(zip(cfg.names, refs, strict=True)))
    n, rows, latent, shift, layers = cfg.n, cfg.rows, cfg.latent, cfg.shift, cfg.layers
    nvar, in_feat = cfg.nvar, cfg.in_feat
    cols_j = n * rows // shift
    nblk = shift // n
    quarter = cols_j // 4
    grid_rows = RATIO * rows
    per_blk = OFFSETS * cols_j
    bpc = 2
    chunk = bpc * per_blk
    nchunk = nblk // bpc
    pair = nblk // 2
    chunks = [(2 * i + 1, 2 * i + 2) for i in range(pair // 2 - 1)] + [(0, pair - 1)] + [(pair + 2 * i, pair + 2 * i + 1) for i in range(pair // 2)]
    flat = [p for c in chunks for p in c]
    me = lax.axis_index("gp")
    left = lax.rem(me + n - 1, n)
    right = lax.rem(me + 1, n)
    pre, hid, ys = (r.p0, r.p1), (r.h0, r.h1), (r.y0, r.y1)

    def remote(src, dst, send, recv, dev):
        return pltpu.make_async_remote_copy(src_ref=src, dst_ref=dst, send_sem=send, recv_sem=recv, device_id={"gp": dev}, device_id_type=pl.DeviceIdType.MESH)

    last = layers + 1
    pairs = dict(
        mfr=(r.mf_h, r.mfr), mer=(r.me_h, r.mer), g2r=(r.g2_h, r.g2r), m2r=(r.m2_h, r.m2r), gsr=(r.gs_h, r.gsr), frr=(r.fr_h, r.frr), nsr=(r.ns_h, r.nsr),
        wmr=(r.wm_h, r.wmr), wer=(r.we_h, r.wer), xp=(r.xp_h, r.xs.at[0]), xc=(r.xc_h, r.xs.at[1]), wg=(r.wg_h, r.wg.at[0:in_feat]), wemb=(r.wemb_h, r.wemb),
        wi1=(r.wei_h.at[last], r.wi.at[1]), wi0=(r.wei_h.at[0], r.wi.at[0]), ni0=(r.wni_h.at[0], r.ni.at[0]), wo0=(r.weo_h.at[0], r.wo.at[0]), no0=(r.wno_h.at[0], r.no.at[0]),
        wself=(r.wself_h, r.wself), wo1=(r.weo_h.at[last], r.wo.at[1]), ni1=(r.wni_h.at[last], r.ni.at[1]), no1=(r.wno_h.at[last], r.no.at[1]), woh=(r.woh_h, r.woh), wof=(r.wof_h, r.wof),
    )
    load = types.SimpleNamespace(**{key: pltpu.make_async_copy(src, dst, r.load_sem.at[i]) for i, (key, (src, dst)) in enumerate(pairs.items())})

    def fetch(layer, slot):
        pairs = ((r.wei_h, r.lwi), (r.weo_h, r.lwo), (r.wni_h, r.lni), (r.wno_h, r.lno))
        return [pltpu.make_async_copy(src.at[layer], dst.at[slot], r.fetch_sem.at[slot, i]) for i, (src, dst) in enumerate(pairs)]

    for c in vars(load).values():
        c.start()
    for c in fetch(1, 0):
        c.start()

    barrier = pltpu.get_barrier_semaphore()
    for off in range(1, n):
        pl.semaphore_signal(barrier, inc=1, device_id={"gp": lax.rem(me + off, n)}, device_id_type=pl.DeviceIdType.MESH)

    def iota(shape, dim):
        return lax.broadcasted_iota(jnp.int32, shape, dim)

    def onehot(pred):
        return jnp.where(pred, 1.0, 0.0).astype(BF16)

    def slot_of(row):
        jp = lax.rem(lax.rem(row, cols_j) + (cols_j - 1), cols_j)
        return jp * nblk + lax.rem(lax.div(row, cols_j) + 1, nblk)

    for t in range(rows // 128):
        sl = slice(128 * t, 128 * t + 128)
        r.pfwd[sl, :] = onehot(iota((128, rows), 1) == slot_of(iota((128, rows), 0) + 128 * t))
        slot = slot_of(iota((128, rows), 1))
        jp = lax.div(slot, nblk)
        slot = lax.rem(jp, 2) * (rows // 2) + lax.div(jp, 2) * nblk + lax.rem(slot, nblk)
        r.pbwd[sl, :] = onehot(iota((128, rows), 0) + 128 * t == slot)
    half = rows // 2
    r.ex[...] = onehot(lax.div(iota((rows, half), 0), RATIO) == iota((rows, half), 1))
    r.ps[...] = onehot(iota((half, rows), 0) == lax.div(iota((half, rows), 1), RATIO))
    for ref in (r.s0, r.sup, r.sdn, r.rr, r.n1, r.edge_s, r.keep, r.esum):
        ref[...] = jnp.zeros(ref.shape, ref.dtype)
    r.wg[in_feat:, :] = jnp.zeros((r.wg.shape[0] - in_feat, latent), BF16)

    def act(p, count, hidden, add=None):
        for o in range(0, count, SLAB):
            x = p[o:o + SLAB, :]
            if add is not None:
                x = x + add(o)
            hidden[o:o + SLAB, :] = silu(x).astype(BF16)

    def finish(y, count, store):
        for o in range(0, count, SLAB):
            store(o, layer_norm(y[o:o + SLAB, :]))

    st = r.p0
    wide = grid_rows // latent

    def staged(value, count=16):
        st[0:count, :] = jnp.zeros((count, latent), F32)
        st[0:value.shape[0], :] = value.astype(F32)
        return st[0:count, :].astype(BF16)

    for c in (load.mfr, load.mer, load.g2r, load.m2r, load.gsr, load.frr, load.nsr, load.wmr, load.wer):
        c.wait()
    r.ew[0] = staged(r.wmr[...])
    for i in range(3):
        r.ew[i + 1] = staged(r.wer[i])
    for i in range(wide):
        at = slice(i * latent, (i + 1) * latent)
        r.gm[0, :, at] = staged(r.g2r[:, at])
        r.gm[1, :, at] = staged(r.m2r[:, at])
    r.mf[32:48, :] = staged(r.mfr[...])
    st[0:32, :] = jnp.zeros((32, latent), F32)
    for k in range(OFFSETS):
        st[4 * k:4 * k + 4, :] = r.mer[k]
    r.mf[0:32, :] = st[0:32, :].astype(BF16)
    force = r.frr.shape[0]
    for i in range(2):
        r.fs[i, 0:force, :] = r.frr[:, i, :]
        r.fs[i, force:force + r.gsr.shape[0], :] = r.gsr[...]
    st[0:128, :] = jnp.zeros((128, latent), F32)
    st[0:4, 0:nvar] = r.nsr[...]
    r.ns[...] = jnp.transpose(st[0:128, 0:256])
    eye = onehot(iota((32, 128), 0) == iota((32, 128), 1))
    r.feat[...] = dot_t(r.mf[0:32, :], eye).astype(BF16).reshape(2, half, 128)
    def grid_embed(s, base):
        at = pl.ds(base, rows)
        mean, std = (r.ns[0:nvar, i:i + 1] for i in (0, 1))
        p = r.p0
        p[0:nvar, :] = (r.xs[s, :, at] - mean) / std
        p[nvar:2 * nvar, :] = (r.xs[1 - s, :, at] - mean) / std
        p[2 * nvar:in_feat, :] = r.fs[s, 0:in_feat - 2 * nvar, at]
        p[in_feat:, :] = jnp.zeros((p.shape[0] - in_feat, rows), F32)
        r.h0[...] = p[...].astype(BF16)
        r.p1[...] = dot_t(r.h0[...], r.wg[...])
        act(r.p1, rows, r.h1)
        r.y1[...] = dot(r.h1[...], r.wemb[0])

        def store(o, v):
            r.gl[pl.ds(base + o, SLAB), :] = v.astype(BF16)

        finish(r.y1, rows, store)

    def first_embed(q, _):
        grid_embed(0, pl.multiple_of(q * rows, rows))
        return 0

    for c in (load.xp, load.xc, load.wg, load.wemb):
        c.wait()
    lax.fori_loop(0, RATIO, first_embed, 0)
    pl.semaphore_wait(barrier, n - 1)

    def feat_copy(off, jj, dev, owner):
        slot = lax.rem(2 * owner + jj + cols_j - 1, cols_j)
        return remote(r.feat.at[jj, pl.ds(pl.multiple_of(nblk * dev, nblk), nblk), :], r.fin.at[slot], r.fsend.at[off, jj], r.frecv.at[off, jj], dev)

    nb_copies = [
        remote(r.mf.at[32:48, 0:half], r.mfp.at[:, half:], r.nsend.at[0], r.nrecv.at[0], left),
        remote(r.gm.at[0, :, 0:rows], r.g2p.at[:, rows:], r.nsend.at[1], r.nrecv.at[1], left),
    ]
    for c in nb_copies:
        c.start()
    for off in range(1, n):
        for jj in range(2):
            feat_copy(off, jj, lax.rem(me + off, n), me).start()
    for jj in range(2):
        r.fin[lax.rem(2 * me + jj + cols_j - 1, cols_j)] = r.feat[jj, pl.ds(pl.multiple_of(nblk * me, nblk), nblk), :]
    r.mfp[:, 0:half] = r.mf[32:48, half:]
    r.g2p[:, 0:rows] = r.gm[0, :, rows:]


    def embed(lhs_t, w_first, w_second, store):
        r.p0[0:rows, :] = dot_t(lhs_t, w_first)
        act(r.p0, rows, r.h0)
        r.y0[0:rows, :] = dot(r.h0[0:rows, :], w_second)
        finish(r.y0, rows, store)

    load.wi1.wait()

    def m2g_body(q, _):
        base = pl.multiple_of(q * rows, rows)

        def store(o, v):
            r.m2g[pl.ds(base + o, SLAB), :] = v.astype(BF16)

        embed(r.gm[1, :, pl.ds(base, rows)], r.ew[2], r.wemb[3], store)
        r.decst[pl.ds(base, rows), :] = dot(r.m2g[pl.ds(base, rows), :], r.wi[1, 0:latent, :])
        return 0

    lax.fori_loop(0, RATIO, m2g_body, 0)

    for c in nb_copies:
        c.wait()
    load.wi0.wait()
    load.ni0.wait()

    def store_mesh(o, v):
        r.mlat[o:o + SLAB, :] = v.astype(BF16)

    embed(r.mfp[...], r.ew[0], r.wemb[1], store_mesh)
    r.nodst[...] = dot(r.mlat[...], r.ni[0, 0:latent, :])

    def g2m_body(q, _):
        base = pl.multiple_of(q * rows, rows)
        hbase = pl.multiple_of(q * half, half)

        def store(o, v):
            r.g2m[pl.ds(base + o, SLAB), :] = v.astype(BF16)

        embed(r.g2p[:, pl.ds(base, rows)], r.ew[1], r.wemb[2], store)
        r.h1[0:rows, :] = dot(r.ex[...], r.mlat[pl.ds(hbase, half), :]).astype(BF16)
        r.encst[pl.ds(base, rows), :] = dot(r.g2m[pl.ds(base, rows), :], r.wi[0, 0:latent, :]) + dot(r.h1[0:rows, :], r.wi[0, 2 * latent:, :])
        return 0


    for c in (load.wo0, load.no0, load.wself):
        c.wait()

    def late_static():
        for c in (load.wo1, load.ni1, load.no1, load.woh, load.wof):
            c.wait()
        for off in range(1, n):
            for jj in range(2):
                feat_copy(off, jj, lax.rem(me + off, n), lax.rem(me + n - off, n)).wait()
        r.featm[...] = dot(r.pfwd[...], r.fin[...].reshape(rows, 128)).astype(BF16)

        def edge_body(k, _):
            sel = onehot(iota((128, 16), 0) == iota((128, 16), 1) + 4 * k)
            sel = jnp.where(iota((128, 16), 1) < 4, sel, jnp.zeros_like(sel))
            w_k = dot(sel, r.ew[3]).astype(BF16)
            r.p0[0:rows, :] = dot(r.featm[...], w_k)
            act(r.p0, rows, r.h0)
            r.y0[0:rows, :] = dot(r.h0[0:rows, :], r.wemb[4])

            def store(o, v):
                pos = flat.index(o // cols_j)
                at = pl.multiple_of(pos * per_blk + (o % cols_j // SLAB * OFFSETS + k) * SLAB, SLAB)
                r.ebase[pl.ds(at, SLAB), :] = v.astype(BF16)

            finish(r.y0, rows, store)
            return 0

        lax.fori_loop(0, OFFSETS, edge_body, 0)

    far_first = sorted(range(1, n), key=lambda off: -min(off, n - off))

    def to_blocks(off, q, dev, owner):
        return remote(r.mcur.at[q, pl.ds(pl.multiple_of(nblk * dev, nblk), nblk), :], r.hin.at[2 * owner + q], r.asend.at[off, q], r.arecv.at[off, q], dev)

    def to_grid(off, q, dev, owner):
        return remote(r.yout.at[q, dev], r.hb.at[q, pl.ds(pl.multiple_of(nblk * owner, nblk), nblk), :], r.bsend.at[off, q], r.brecv.at[off, q], dev)

    def encode(q):
        base = pl.multiple_of(q * rows, rows)
        at = pl.ds(base, rows)
        r.p0[...] = dot(r.gl[at, :], r.wi[0, latent:2 * latent, :])
        act(r.p0, rows, r.h0, lambda o: r.encst[pl.ds(base + o, SLAB), :])
        r.y0[...] = dot(r.h0[...], r.wo[0])

        def store_edge(o, v):
            r.h1[o:o + SLAB, :] = (r.g2m[pl.ds(base + o, SLAB), :].astype(F32) + v).astype(BF16)

        finish(r.y0, rows, store_edge)
        hbase = pl.multiple_of(q * half, half)
        esum = dot(r.ps[...], r.h1[...]).astype(BF16)
        r.p1[0:half, :] = dot(esum, r.ni[0, latent:, :])
        act(r.p1, half, r.h0, lambda o: r.nodst[pl.ds(hbase + o, SLAB), :])
        r.y1[0:half, :] = dot(r.h0[0:half, :], r.no[0])

        def store_node(o, v):
            r.mcur[q, o:o + SLAB, :] = (r.mlat[pl.ds(hbase + o, SLAB), :].astype(F32) + v).astype(BF16)

        finish(r.y1, half, store_node)
        for off in far_first:
            to_blocks(off, q, lax.rem(me + off, n), me).start()
        r.hin[2 * me + q] = r.mcur[q, pl.ds(pl.multiple_of(nblk * me, nblk), nblk), :]

    s0, sup, sdn, rr, n1, e, h, esum = r.s0, r.sup, r.sdn, r.rr, r.n1, r.e, r.h, r.esum
    npre, nhid, nys = r.np, r.nh, r.ny
    group = rows // 2

    def halo_copies(par):
        lo, hi = (nblk - 2) * cols_j, (nblk - 1) * cols_j
        return [
            remote(s0.at[lo:lo + cols_j], r.halo.at[par, 0], r.hsend.at[0], r.hrecv.at[par, 0], right),
            remote(s0.at[hi:hi + cols_j], r.halo.at[par, 1], r.hsend.at[1], r.hrecv.at[par, 1], left),
        ]

    def take_halo(par):
        for c in halo_copies(par):
            c.wait()
        low, high = r.halo[par, 0], r.halo[par, 1]
        low_w = jnp.concatenate([low[-1:], low[:-1]], axis=0)
        high_w = jnp.concatenate([high[1:], high[:1]], axis=0)
        r.edge_s[0] = jnp.where(me == 0, low_w, low)
        r.edge_s[1] = jnp.where(me == n - 1, high_w, high)

    def send(p, k, g):
        at = slice(SLAB * g, SLAB * g + SLAB)
        if k == 0:
            if p == nblk - 2:
                return r.edge_s[1, at, :]
            if p == nblk - 1:
                return r.keep[at, :]
            base = (p + 1) % nblk * cols_j
            return s0[base + SLAB * g:base + SLAB * g + SLAB, :]
        if k == 1:
            if p == nblk - 1:
                return r.edge_s[0, at, :]
            base = (p - 1) % nblk * cols_j
            return s0[base + SLAB * g:base + SLAB * g + SLAB, :]
        base = p * cols_j
        if k in (2, 3):
            return (sup, sdn)[k - 2][base + SLAB * g:base + SLAB * g + SLAB, :]
        sh = quarter if k == 4 else -quarter
        lo, hi = (SLAB * g + sh) % cols_j, (SLAB * g + 8 + sh) % cols_j
        return jnp.concatenate([s0[base + lo:base + lo + 8, :], s0[base + hi:base + hi + 8, :]], axis=0)

    def edge_act(i):
        for bb, p in enumerate(chunks[i]):
            for g in range(cols_j // SLAB):
                recv = rr[p * cols_j + SLAB * g:p * cols_j + SLAB * g + SLAB, :]
                for k in range(OFFSETS):
                    o = bb * per_blk + (g * OFFSETS + k) * SLAB
                    hid[i % 2][o:o + SLAB, :] = silu(pre[i % 2][o:o + SLAB, :] + send(p, k, g) + recv).astype(BF16)

    def edge_finish(i):
        rows6 = OFFSETS * SLAB
        for bb, p in enumerate(chunks[i]):
            for g in range(cols_j // SLAB):
                o = bb * per_blk + g * rows6
                eo = i * chunk + o
                new = (e[eo:eo + rows6, :].astype(F32) + layer_norm(ys[i % 2][o:o + rows6, :])).astype(BF16)
                e[eo:eo + rows6, :] = new
                total = new[0:SLAB].astype(F32)
                for k in range(1, OFFSETS):
                    total = total + new[k * SLAB:(k + 1) * SLAB].astype(F32)
                esum[p * cols_j + SLAB * g:p * cols_j + SLAB * g + SLAB, :] = total.astype(BF16)

    def edge_first(i, wi):
        pre[i % 2][0:chunk, :] = dot(e[i * chunk:(i + 1) * chunk, :], wi[0:latent, :])

    def edge_second(i, wo):
        ys[i % 2][0:chunk, :] = dot(hid[i % 2][0:chunk, :], wo[...])

    groups = ((0, group), (group, group // 2), (group + group // 2, group // 2))

    def project_send(g, wi):
        o, count = groups[g]
        s0[o:o + count, :] = dot(h[o:o + count, :], wi[latent:2 * latent, :])

    def roll_send(g):
        o, count = groups[g]
        for at in range(o, o + count, cols_j):
            blk = s0[at:at + cols_j, :]
            sup[at:at + cols_j, :] = jnp.concatenate([blk[1:], blk[:1]], axis=0)
            sdn[at:at + cols_j, :] = jnp.concatenate([blk[-1:], blk[:-1]], axis=0)

    def project_rest(g, wi, ni):
        o, count = groups[g]
        rr[o:o + count, :] = dot(h[o:o + count, :], wi[2 * latent:, :])
        n1[o:o + count, :] = dot(h[o:o + count, :], ni[0:latent, :])

    def node_first(g, ni):
        o, count = groups[g]
        npre[o:o + count, :] = dot(esum[o:o + count, :], ni[latent:, :])

    def node_act(g):
        o, count = groups[g]
        for at in range(o, o + count, SLAB):
            nhid[at:at + SLAB, :] = silu(npre[at:at + SLAB, :] + n1[at:at + SLAB, :]).astype(BF16)

    def node_second(g, no):
        o, count = groups[g]
        nys[o:o + count, :] = dot(nhid[o:o + count, :], no[...])

    def node_finish(g):
        o, count = groups[g]
        step = 4 * SLAB
        for at in range(o, o + count, step):
            h[at:at + step, :] = (h[at:at + step, :].astype(F32) + layer_norm(nys[at:at + step, :])).astype(BF16)

    def weights(i):
        return [x.at[i] for x in (r.lwi, r.lwo, r.lni, r.lno)]

    def layer_body(t, first):
        cur, was, nxt = (lax.rem(first + t + i, 3) for i in (0, 2, 1))
        par = lax.rem(first + t, 2)
        wi, wo, ni, no = weights(cur)
        wi_n, _, ni_n, _ = weights(nxt)
        _, wo_w, ni_w, no_w = weights(was)

        @pl.when(t > 0)
        def _():
            take_halo(1 - par)

        def run(stages, table):
            for stage in stages:
                name = stage.rstrip("0123456789")
                table[name](*(int(d) for d in stage[len(name):]))

        last_chunk = nchunk - 1
        run(LOWER, dict(
            A=edge_act, E=edge_finish, F=lambda i: edge_first(i, wi), S=lambda i: edge_second(i, wo_w if i == last_chunk else wo),
            nf=lambda g: node_first(g, ni_w), na=node_act, ns=lambda g: node_second(g, no_w), ne=node_finish,
            ps=lambda g: project_send(g, wi), ro=roll_send))
        for c in halo_copies(par):
            c.start()
        for c in fetch(jnp.where(t + 1 < layers, t + 2, 1), nxt):
            c.wait()
        for c in fetch(jnp.where(t + 2 < layers, t + 3, t + 3 - layers), was):
            c.start()

        def keep():
            r.keep[...] = s0[0:cols_j, :]

        run(UPPER, dict(
            A=edge_act, E=edge_finish, F=lambda i: edge_first(i, wi), S=lambda i: edge_second(i, wo),
            nf=lambda g: node_first(g, ni), na=node_act, ns=lambda g: node_second(g, no), ne=node_finish,
            ps=lambda g: project_send(g, wi if g else wi_n), pr=lambda g: project_rest(g, wi if g else wi_n, ni if g else ni_n), ro=roll_send, KEEP=keep))
        return first

    def run_layers(first):
        was, cur = (lax.rem(first + i, 3) for i in (2, 0))
        wi, _, ni, _ = weights(cur)
        r.lwo[was] = jnp.zeros((latent, latent), BF16)
        r.lno[was] = jnp.zeros((latent, latent), BF16)
        r.lni[was, latent:, :] = jnp.zeros((latent, latent), BF16)
        r.y0[...] = jnp.zeros(r.y0.shape, F32)
        project_send(0, wi)
        roll_send(0)
        project_rest(0, wi, ni)
        lax.fori_loop(0, layers, layer_body, first)
        was = lax.rem(first + layers + 2, 3)
        take_halo(lax.rem(first + layers + 1, 2))
        edge_act(7)
        edge_second(7, r.lwo.at[was])
        edge_finish(6)
        edge_finish(7)
        for g in (1, 2):
            node_first(g, r.lni.at[was])
            node_act(g)
            node_second(g, r.lno.at[was])
            node_finish(g)

    def step_body(s, _):
        x_prev, x_cur = r.xs.at[s], r.xs.at[1 - s]
        dmean, dstd = (r.ns[0:nvar, i:i + 1] for i in (2, 3))

        def self_body(q, _):
            base = pl.multiple_of(q * rows, rows)
            at = pl.ds(base, rows)
            r.p0[...] = dot(r.gl[at, :], r.wself[0])
            act(r.p0, rows, r.h0)
            r.y0[...] = dot(r.h0[...], r.wself[1])

            def store(o, v):
                w = pl.ds(base + o, SLAB)
                r.gcur[w, :] = (r.gl[w, :].astype(F32) + v).astype(BF16)

            finish(r.y0, rows, store)
            return 0

        lax.fori_loop(0, RATIO, self_body, 0)
        pl.when(s == 0)(late_static)

        def copy_body(i, _):
            at = pl.ds(pl.multiple_of(i * chunk, chunk), chunk)
            r.e[at, :] = r.ebase[at, :]
            return 0

        lax.fori_loop(0, nchunk, copy_body, 0)
        for q in range(2):
            for off in far_first:
                to_blocks(off, q, lax.rem(me + off, n), lax.rem(me + n - off, n)).wait()
        r.h[...] = dot(r.pfwd[...], r.hin[...].reshape(rows, latent)).astype(BF16)

        run_layers(s * layers)

        for q in range(2):
            r.yout[q] = dot(r.pbwd[q * half:(q + 1) * half, :], r.h[...]).astype(BF16).reshape(n, nblk, latent)
            for off in far_first:
                to_grid(off, q, lax.rem(me + off, n), me).start()
            r.hb[q, pl.ds(pl.multiple_of(nblk * me, nblk), nblk), :] = r.yout[q, me]

        def dec_body(q, _):
            base = pl.multiple_of(q * rows, rows)
            at = pl.ds(base, rows)
            for off in far_first:
                to_grid(off, q, lax.rem(me + off, n), lax.rem(me + n - off, n)).wait()
            r.h1[...] = dot(r.ex[...], r.hb[q]).astype(BF16)
            r.p0[...] = dot(r.h1[...], r.wi[1, latent:2 * latent, :]) + dot(r.gcur[at, :], r.wi[1, 2 * latent:, :])
            act(r.p0, rows, r.h0, lambda o: r.decst[pl.ds(base + o, SLAB), :])
            r.y0[...] = dot(r.h0[...], r.wo[1])

            def store_edge(o, v):
                r.h1[o:o + SLAB, :] = (r.m2g[pl.ds(base + o, SLAB), :].astype(F32) + v).astype(BF16)

            finish(r.y0, rows, store_edge)
            r.p1[...] = dot(r.gcur[at, :], r.ni[1, 0:latent, :]) + dot(r.h1[...], r.ni[1, latent:, :])
            act(r.p1, rows, r.h0)
            r.y1[...] = dot(r.h0[...], r.no[1])

            def store_node(o, v):
                r.h1[o:o + SLAB, :] = (r.gcur[pl.ds(base + o, SLAB), :].astype(F32) + v).astype(BF16)

            finish(r.y1, rows, store_node)
            r.p0[...] = dot(r.h1[...], r.woh[...])
            act(r.p0, rows, r.h0)
            pred = dot_bt(r.wof[...], r.h0[...])
            x_prev[:, at] = x_cur[:, at] + dstd * pred + dmean

            @pl.when(s == 0)
            def _():
                grid_embed(1, base)
                encode(q)

            return 0

        lax.fori_loop(0, RATIO, dec_body, 0)
        for i, out in enumerate((r.out_a, r.out_b)):

            @pl.when(s == i)
            def _(i=i, out=out):
                pltpu.make_async_copy(r.xs.at[i], out, r.out_sem.at[i]).start()

        return 0

    for c in fetch(1, 0):
        c.wait()
    for c in fetch(2, 1):
        c.start()
    def first_encode(q, _):
        g2m_body(q, 0)
        encode(q)
        return 0

    lax.fori_loop(0, RATIO, first_encode, 0)
    lax.fori_loop(0, 2, step_body, 0)
    for i, out in enumerate((r.out_a, r.out_b)):
        pltpu.make_async_copy(r.xs.at[i], out, r.out_sem.at[i]).wait()
    for c in fetch(1, (2 * layers + 1) % 3):
        c.wait()


def solution(mesh):
    n = mesh.shape["gp"]
    row_spec = P(("dp", "gp"))
    edge_spec = P(("dp", "gp"), None, None)
    whole = P()

    def local_run(x_prev, x_cur, forcing, grid_static, g2m_feat, m2g_feat, mesh_feat, mesh_edge_feat, norm_stats, w_grid_in, w_mesh_in, w_eemb_in, w_embed_out, w_edge_in, w_edge_out, w_node_in, w_node_out, w_grid_self, w_out_hidden, w_out_final):
        grid_rows, nvar = x_prev.shape
        rows = mesh_feat.shape[0]
        latent = w_embed_out.shape[-1]
        blocks = w_edge_in.shape[0]
        in_feat = w_grid_in.shape[0]
        shift = rows // 2
        cols_j = n * rows // shift
        nblk = shift // n
        chunk = 2 * OFFSETS * cols_j

        inputs = dict(xp_h=x_prev.T, xc_h=x_cur.T, fr_h=forcing.transpose(2, 1, 0), gs_h=grid_static.T, g2_h=g2m_feat.T, m2_h=m2g_feat.T, mf_h=mesh_feat.T, me_h=mesh_edge_feat.transpose(1, 2, 0), ns_h=norm_stats, wm_h=w_mesh_in, we_h=w_eemb_in, wg_h=w_grid_in, wemb_h=w_embed_out, wei_h=w_edge_in, weo_h=w_edge_out, wni_h=w_node_in, wno_h=w_node_out, wself_h=w_grid_self, woh_h=w_out_hidden, wof_h=w_out_final.T)
        big = max(rows, chunk)
        vm = pltpu.VMEM
        dma = pltpu.SemaphoreType.DMA
        scratch = dict(
            xs=vm((2, nvar, grid_rows), F32), fs=vm((2, 16, grid_rows), F32), ns=vm((256, 128), F32), gm=vm((2, 16, grid_rows), BF16), mf=vm((48, rows), BF16),
            ew=vm((4, 16, latent), BF16), wg=vm((rows, latent), BF16), wemb=vm(w_embed_out.shape, BF16),
            wi=vm((2, 3 * latent, latent), BF16), wo=vm((2, latent, latent), BF16), ni=vm((2, 2 * latent, latent), BF16), no=vm((2, latent, latent), BF16),
            wself=vm(w_grid_self.shape, BF16), woh=vm(w_out_hidden.shape, BF16),
            lwi=vm((3, 3 * latent, latent), BF16), lwo=vm((3, latent, latent), BF16), lni=vm((3, 2 * latent, latent), BF16), lno=vm((3, latent, latent), BF16),
            pfwd=vm((rows, rows), BF16), pbwd=vm((rows, rows), BF16), ex=vm((rows, rows // 2), BF16), ps=vm((rows // 2, rows), BF16),
            feat=vm((2, rows // 2, 128), BF16), fin=vm((cols_j, nblk, 128), BF16), featm=vm((rows, 128), BF16), mfp=vm((16, rows), BF16), g2p=vm((16, grid_rows), BF16),
            m2g=vm((grid_rows, latent), BF16), g2m=vm((grid_rows, latent), BF16), mlat=vm((rows, latent), BF16),
            decst=vm((grid_rows, latent), F32), encst=vm((grid_rows, latent), F32), nodst=vm((rows, latent), F32),
            gl=vm((grid_rows, latent), BF16), gcur=vm((grid_rows, latent), BF16), mcur=vm((2, rows // 2, latent), BF16),
            hin=vm((cols_j, nblk, latent), BF16), hb=vm((2, rows // 2, latent), BF16), yout=vm((2, n, nblk, latent), BF16),
            ebase=vm((OFFSETS * rows, latent), BF16), e=vm((OFFSETS * rows, latent), BF16), h=vm((rows, latent), BF16),
            s0=vm((rows, latent), F32), sup=vm((rows, latent), F32), sdn=vm((rows, latent), F32), rr=vm((rows, latent), F32), n1=vm((rows, latent), F32),
            esum=vm((rows, latent), BF16), edge_s=vm((2, cols_j, latent), F32), keep=vm((cols_j, latent), F32), np=vm((rows, latent), F32), nh=vm((rows, latent), BF16), ny=vm((rows, latent), F32), halo=vm((2, 2, cols_j, latent), F32),
            p0=vm((big, latent), F32), p1=vm((big, latent), F32), h0=vm((big, latent), BF16), h1=vm((big, latent), BF16), y0=vm((big, latent), F32), y1=vm((big, latent), F32),
            wof=vm((nvar, latent), BF16), mfr=vm((mesh_feat.shape[1], rows), F32), mer=vm((*mesh_edge_feat.shape[1:], rows), F32), g2r=vm((g2m_feat.shape[1], grid_rows), F32), m2r=vm((m2g_feat.shape[1], grid_rows), F32),
            gsr=vm((grid_static.shape[1], grid_rows), F32), frr=vm((forcing.shape[2], forcing.shape[1], grid_rows), F32), nsr=vm(norm_stats.shape, F32), wmr=vm(w_mesh_in.shape, BF16), wer=vm(w_eemb_in.shape, BF16),
            load_sem=dma((24,)), fetch_sem=dma((3, 4)), out_sem=dma((2,)), fsend=dma((n, 2)), frecv=dma((n, 2)), nsend=dma((2,)), nrecv=dma((2,)),
            asend=dma((n, 2)), arecv=dma((n, 2)), bsend=dma((n, 2)), brecv=dma((n, 2)), hsend=dma((2,)), hrecv=dma((2, 2)),
        )
        cfg = types.SimpleNamespace(names=(*inputs, "out_a", "out_b", *scratch), n=n, rows=rows, latent=latent, shift=shift, layers=blocks - 2, nvar=nvar, in_feat=in_feat)
        anywhere = pl.BlockSpec(memory_space=pl.ANY)
        out = pl.pallas_call(
            functools.partial(kernel, cfg),
            out_shape=[jax.ShapeDtypeStruct((nvar, grid_rows), F32)] * 2,
            in_specs=[anywhere] * len(inputs),
            out_specs=[anywhere] * 2,
            scratch_shapes=list(scratch.values()),
            compiler_params=pltpu.CompilerParams(collective_id=0, has_side_effects=True, vmem_limit_bytes=66_000_000),
        )(*inputs.values())
        return out[0].T, out[1].T

    in_specs = (row_spec, row_spec, edge_spec, row_spec, row_spec, row_spec, row_spec, edge_spec, whole) + (whole,) * 11
    return jax.shard_map(local_run, mesh=mesh, in_specs=in_specs, out_specs=(row_spec, row_spec), check_vma=False)
```

```python
import functools
import types

import jax
import jax.numpy as jnp
from jax import lax
from jax.experimental import pallas as pl
from jax.experimental.pallas import tpu as pltpu
from jax.sharding import PartitionSpec as P

F32 = jnp.float32
BF16 = jnp.bfloat16
SLAB = 16
GROUP = 64
RATIO = 2
OFFSETS = 6
LOWER = ("E6", "A7", "S7", "F0", "F1", "A0", "nf1", "E7", "na1", "nf2", "na2", "A1", "ns2", "S0", "F3", "E0", "ne2", "ns1", "F2", "ne1", "S1", "A2", "E1", "S2", "ps2")
UPPER = ("ro2", "ps1", "E2", "ro1", "pr1", "A3", "S3", "pr2", "F4", "A4", "E3", "F5", "F6", "S4", "nf0", "A5", "na0", "S5", "ns0", "E4", "A6", "ne0", "KEEP", "S6", "E5", "F7", "ps0", "ro0", "pr0")


def dot(a, b):
    return jnp.dot(a, b, preferred_element_type=F32)


def dot_t(a, b):
    return lax.dot_general(a, b, (((0,), (0,)), ((), ())), preferred_element_type=F32)


def dot_bt(a, b):
    return lax.dot_general(a, b, (((1,), (1,)), ((), ())), preferred_element_type=F32)


def silu(x):
    return x * lax.logistic(x)


def layer_norm(y):
    centred = y - jnp.mean(y, axis=-1, keepdims=True)
    spread = jnp.mean(centred * centred, axis=-1, keepdims=True)
    return centred * lax.rsqrt(spread + 1e-5)


def kernel(cfg, *refs):
    r = types.SimpleNamespace(**dict(zip(cfg.names, refs, strict=True)))
    n, rows, latent, shift, layers = cfg.n, cfg.rows, cfg.latent, cfg.shift, cfg.layers
    nvar, in_feat = cfg.nvar, cfg.in_feat
    cols_j = n * rows // shift
    nblk = shift // n
    quarter = cols_j // 4
    grid_rows = RATIO * rows
    per_blk = OFFSETS * cols_j
    bpc = 2
    chunk = bpc * per_blk
    nchunk = nblk // bpc
    pair = nblk // 2
    chunks = [(2 * i + 1, 2 * i + 2) for i in range(pair // 2 - 1)] + [(0, pair - 1)] + [(pair + 2 * i, pair + 2 * i + 1) for i in range(pair // 2)]
    flat = [p for c in chunks for p in c]
    me = lax.axis_index("gp")
    left = lax.rem(me + n - 1, n)
    right = lax.rem(me + 1, n)
    pre, hid, ys = (r.p0, r.p1), (r.h0, r.h1), (r.y0, r.y1)

    def remote(src, dst, send, recv, dev):
        return pltpu.make_async_remote_copy(src_ref=src, dst_ref=dst, send_sem=send, recv_sem=recv, device_id={"gp": dev}, device_id_type=pl.DeviceIdType.MESH)

    last = layers + 1
    pairs = dict(
        mfr=(r.mf_h, r.mfr), mer=(r.me_h, r.mer), g2r=(r.g2_h, r.g2r), m2r=(r.m2_h, r.m2r), gsr=(r.gs_h, r.gsr), frr=(r.fr_h, r.frr), nsr=(r.ns_h, r.nsr),
        wmr=(r.wm_h, r.wmr), wer=(r.we_h, r.wer), xp=(r.xp_h, r.xs.at[0]), xc=(r.xc_h, r.xs.at[1]), wg=(r.wg_h, r.wg.at[0:in_feat]), wemb=(r.wemb_h, r.wemb),
        wi1=(r.wei_h.at[last], r.wi.at[1]), wi0=(r.wei_h.at[0], r.wi.at[0]), ni0=(r.wni_h.at[0], r.ni.at[0]), wo0=(r.weo_h.at[0], r.wo.at[0]), no0=(r.wno_h.at[0], r.no.at[0]),
        wself=(r.wself_h, r.wself), wo1=(r.weo_h.at[last], r.wo.at[1]), ni1=(r.wni_h.at[last], r.ni.at[1]), no1=(r.wno_h.at[last], r.no.at[1]), woh=(r.woh_h, r.woh), wof=(r.wof_h, r.wof),
    )
    load = types.SimpleNamespace(**{key: pltpu.make_async_copy(src, dst, r.load_sem.at[i]) for i, (key, (src, dst)) in enumerate(pairs.items())})

    def fetch(layer, slot):
        pairs = ((r.wei_h, r.lwi), (r.weo_h, r.lwo), (r.wni_h, r.lni), (r.wno_h, r.lno))
        return [pltpu.make_async_copy(src.at[layer], dst.at[slot], r.fetch_sem.at[slot, i]) for i, (src, dst) in enumerate(pairs)]

    for c in vars(load).values():
        c.start()
    for c in fetch(1, 0):
        c.start()

    barrier = pltpu.get_barrier_semaphore()
    for off in range(1, n):
        pl.semaphore_signal(barrier, inc=1, device_id={"gp": lax.rem(me + off, n)}, device_id_type=pl.DeviceIdType.MESH)

    def iota(shape, dim):
        return lax.broadcasted_iota(jnp.int32, shape, dim)

    def onehot(pred):
        return jnp.where(pred, 1.0, 0.0).astype(BF16)

    def slot_of(row):
        jp = lax.rem(lax.rem(row, cols_j) + (cols_j - 1), cols_j)
        return jp * nblk + lax.rem(lax.div(row, cols_j) + 1, nblk)

    half = rows // 2
    r.ex[...] = onehot(lax.div(iota((rows, half), 0), RATIO) == iota((rows, half), 1))
    r.ps[...] = onehot(iota((half, rows), 0) == lax.div(iota((half, rows), 1), RATIO))
    r.wg[in_feat:, :] = jnp.zeros((r.wg.shape[0] - in_feat, latent), BF16)

    def act(p, lo, count, hidden, add=None):
        for o in range(lo, lo + count, SLAB):
            x = p[o:o + SLAB, :]
            if add is not None:
                x = x + add(o)
            hidden[o:o + SLAB, :] = silu(x).astype(BF16)

    def finish(y, lo, count, store):
        for o in range(lo, lo + count, GROUP):
            store(o, layer_norm(y[o:o + GROUP, :]))

    halves = (0, half)

    def chain(*stages):
        for stage in stages:
            for u in halves:
                stage(slice(u, u + half), u)

    st = r.p0
    wide = grid_rows // latent

    def staged(value, count=16):
        st[0:count, :] = jnp.zeros((count, latent), F32)
        st[0:value.shape[0], :] = value.astype(F32)
        return st[0:count, :].astype(BF16)

    for c in (load.mfr, load.mer, load.g2r, load.m2r, load.gsr, load.frr, load.nsr, load.wmr, load.wer):
        c.wait()
    r.ew[0] = staged(r.wmr[...])
    for i in range(3):
        r.ew[i + 1] = staged(r.wer[i])
    for i in range(wide):
        at = slice(i * latent, (i + 1) * latent)
        r.gm[0, :, at] = staged(r.g2r[:, at])
        r.gm[1, :, at] = staged(r.m2r[:, at])
    r.mf[32:48, :] = staged(r.mfr[...])
    st[0:32, :] = jnp.zeros((32, latent), F32)
    for k in range(OFFSETS):
        st[4 * k:4 * k + 4, :] = r.mer[k]
    r.mf[0:32, :] = st[0:32, :].astype(BF16)
    force = r.frr.shape[0]
    for i in range(2):
        r.fs[i, 0:force, :] = r.frr[:, i, :]
        r.fs[i, force:force + r.gsr.shape[0], :] = r.gsr[...]
    st[0:128, :] = jnp.zeros((128, latent), F32)
    st[0:4, 0:nvar] = r.nsr[...]
    r.ns[...] = jnp.transpose(st[0:128, 0:256])
    eye = onehot(iota((32, 128), 0) == iota((32, 128), 1))
    r.feat[...] = dot_t(r.mf[0:32, :], eye).astype(BF16).reshape(2, half, 128)
    def grid_embed(s, base):
        at = pl.ds(base, rows)
        mean, std = (r.ns[0:nvar, i:i + 1] for i in (0, 1))
        p = r.p0
        p[0:nvar, :] = (r.xs[s, :, at] - mean) / std
        p[nvar:2 * nvar, :] = (r.xs[1 - s, :, at] - mean) / std
        p[2 * nvar:in_feat, :] = r.fs[s, 0:in_feat - 2 * nvar, at]
        p[in_feat:, :] = jnp.zeros((p.shape[0] - in_feat, rows), F32)
        r.h0[...] = p[...].astype(BF16)

        def store(o, v):
            r.gl[pl.ds(base + o, GROUP), :] = v.astype(BF16)

        def first(w, u):
            r.p1[w, :] = dot_t(r.h0[:, w], r.wg[...])

        def second(w, u):
            r.y1[w, :] = dot(r.h1[w, :], r.wemb[0])

        chain(first, lambda w, u: act(r.p1, u, half, r.h1), second, lambda w, u: finish(r.y1, u, half, store))

    def first_embed(q, _):
        grid_embed(0, pl.multiple_of(q * rows, rows))
        return 0

    for c in (load.xp, load.xc, load.wg, load.wemb):
        c.wait()
    lax.fori_loop(0, RATIO, first_embed, 0)
    pl.semaphore_wait(barrier, n - 1)

    def feat_copy(off, dev, owner):
        return remote(r.feat.at[:, pl.ds(pl.multiple_of(nblk * dev, nblk), nblk), :], r.fin.at[pl.ds(2 * owner, 2)], r.fsend.at[off], r.frecv.at[off], dev)

    nb_copies = [
        remote(r.mf.at[32:48, 0:half], r.mfp.at[:, half:], r.nsend.at[0], r.nrecv.at[0], left),
        remote(r.gm.at[0, :, 0:rows], r.g2p.at[:, rows:], r.nsend.at[1], r.nrecv.at[1], left),
    ]
    for c in nb_copies:
        c.start()
    for off in range(1, n):
        feat_copy(off, lax.rem(me + off, n), me).start()
    r.fin[pl.ds(2 * me, 2)] = r.feat[:, pl.ds(pl.multiple_of(nblk * me, nblk), nblk), :]
    r.mfp[:, 0:half] = r.mf[32:48, half:]
    r.g2p[:, 0:rows] = r.gm[0, :, rows:]


    def embed(lhs_t, w_first, w_second, store, last=None):
        def first(w, u):
            r.p0[w, :] = dot_t(lhs_t[:, w], w_first)

        def second(w, u):
            r.y0[w, :] = dot(r.h0[w, :], w_second)

        stages = (first, lambda w, u: act(r.p0, u, half, r.h0), second, lambda w, u: finish(r.y0, u, half, store))
        chain(*stages, *(() if last is None else (last,)))

    load.wi1.wait()

    def m2g_body(q, _):
        base = pl.multiple_of(q * rows, rows)

        def store(o, v):
            r.m2g[pl.ds(base + o, GROUP), :] = v.astype(BF16)

        def last(w, u):
            at = pl.ds(base + u, half)
            r.decst[at, :] = dot(r.m2g[at, :], r.wi[1, 0:latent, :])

        embed(r.gm[1, :, pl.ds(base, rows)], r.ew[2], r.wemb[3], store, last)
        return 0

    lax.fori_loop(0, RATIO, m2g_body, 0)

    for c in nb_copies:
        c.wait()
    load.wi0.wait()
    load.ni0.wait()

    def store_mesh(o, v):
        r.mlat[o:o + GROUP, :] = v.astype(BF16)

    def mesh_last(w, u):
        r.nodst[w, :] = dot(r.mlat[w, :], r.ni[0, 0:latent, :])

    embed(r.mfp[...], r.ew[0], r.wemb[1], store_mesh, mesh_last)

    def g2m_body(q):
        base = pl.multiple_of(q * rows, rows)
        hbase = pl.multiple_of(q * half, half)

        def store(o, v):
            r.g2m[pl.ds(base + o, GROUP), :] = v.astype(BF16)

        def last(w, u):
            at = pl.ds(base + u, half)
            r.h1[w, :] = dot(r.ex[0:half, 0:half // 2], r.mlat[pl.ds(hbase + u // 2, half // 2), :]).astype(BF16)
            r.encst[at, :] = dot(r.g2m[at, :], r.wi[0, 0:latent, :]) + dot(r.h1[w, :], r.wi[0, 2 * latent:, :])

        embed(r.g2p[:, pl.ds(base, rows)], r.ew[1], r.wemb[2], store, last)

    for c in (load.wo0, load.no0, load.wself):
        c.wait()

    def late_static():
        for t in range(rows // 128):
            sl = slice(128 * t, 128 * t + 128)
            r.pfwd[sl, :] = onehot(iota((128, rows), 1) == slot_of(iota((128, rows), 0) + 128 * t))
            slot = slot_of(iota((128, rows), 1))
            jp = lax.div(slot, nblk)
            slot = lax.rem(jp, 2) * (rows // 2) + lax.div(jp, 2) * nblk + lax.rem(slot, nblk)
            r.pbwd[sl, :] = onehot(iota((128, rows), 0) + 128 * t == slot)
        for ref in (r.s0, r.sup, r.sdn, r.rr, r.n1, r.edge_s, r.keep, r.esum):
            ref[...] = jnp.zeros(ref.shape, ref.dtype)
        for c in (load.wo1, load.ni1, load.no1, load.woh, load.wof):
            c.wait()
        for off in range(1, n):
            feat_copy(off, lax.rem(me + off, n), lax.rem(me + n - off, n)).wait()
        columns = jnp.concatenate([r.fin[1:], r.fin[0:1]], axis=0)
        r.featm[...] = dot(r.pfwd[...], columns.reshape(rows, 128)).astype(BF16)

        def edge_body(k, _):
            sel = onehot(iota((128, 16), 0) == iota((128, 16), 1) + 4 * k)
            sel = jnp.where(iota((128, 16), 1) < 4, sel, jnp.zeros_like(sel))
            w_k = dot(sel, r.ew[3]).astype(BF16)

            def store(o, v):
                for i in range(0, GROUP, SLAB):
                    pos = flat.index((o + i) // cols_j)
                    at = pl.multiple_of(pos * per_blk + ((o + i) % cols_j // SLAB * OFFSETS + k) * SLAB, SLAB)
                    r.ebase[pl.ds(at, SLAB), :] = v[i:i + SLAB].astype(BF16)

            def first(w, u):
                r.p0[w, :] = dot(r.featm[w, :], w_k)

            def second(w, u):
                r.y0[w, :] = dot(r.h0[w, :], r.wemb[4])

            chain(first, lambda w, u: act(r.p0, u, half, r.h0), second, lambda w, u: finish(r.y0, u, half, store))
            return 0

        lax.fori_loop(0, OFFSETS, edge_body, 0)

    far_first = sorted(range(1, n), key=lambda off: -min(off, n - off))

    def to_blocks(off, q, dev, owner):
        return remote(r.mcur.at[q, pl.ds(pl.multiple_of(nblk * dev, nblk), nblk), :], r.hin.at[2 * owner + q], r.asend.at[off, q], r.arecv.at[off, q], dev)

    def to_grid(off, q, dev, owner):
        return remote(r.yout.at[q, dev], r.hb.at[q, pl.ds(pl.multiple_of(nblk * owner, nblk), nblk), :], r.bsend.at[off, q], r.brecv.at[off, q], dev)

    def encode(q):
        base = pl.multiple_of(q * rows, rows)
        hbase = pl.multiple_of(q * half, half)
        few = half // RATIO

        def edge_one(w, u):
            r.p0[w, :] = dot(r.gl[pl.ds(base + u, half), :], r.wi[0, latent:2 * latent, :])

        def edge_two(w, u):
            r.y0[w, :] = dot(r.h0[w, :], r.wo[0])

        def store_edge(o, v):
            r.h1[o:o + GROUP, :] = (r.g2m[pl.ds(base + o, GROUP), :].astype(F32) + v).astype(BF16)

        def node_one(w, u):
            total = dot(r.ps[0:few, 0:half], r.h1[w, :]).astype(BF16)
            r.p1[u // RATIO:u // RATIO + few, :] = dot(total, r.ni[0, latent:, :])

        def node_two(w, u):
            at = slice(u // RATIO, u // RATIO + few)
            r.y1[at, :] = dot(r.h0[at, :], r.no[0])

        def store_node(o, v):
            r.mcur[q, o:o + GROUP, :] = (r.mlat[pl.ds(hbase + o, GROUP), :].astype(F32) + v).astype(BF16)

        chain(
            edge_one, lambda w, u: act(r.p0, u, half, r.h0, lambda o: r.encst[pl.ds(base + o, SLAB), :]),
            edge_two, lambda w, u: finish(r.y0, u, half, store_edge),
            node_one, lambda w, u: act(r.p1, u // RATIO, few, r.h0, lambda o: r.nodst[pl.ds(hbase + o, SLAB), :]),
            node_two, lambda w, u: finish(r.y1, u // RATIO, few, store_node),
        )
        for off in far_first:
            to_blocks(off, q, lax.rem(me + off, n), me).start()
        r.hin[2 * me + q] = r.mcur[q, pl.ds(pl.multiple_of(nblk * me, nblk), nblk), :]

    s0, sup, sdn, rr, n1, e, h, esum = r.s0, r.sup, r.sdn, r.rr, r.n1, r.e, r.h, r.esum
    npre, nhid, nys = r.np, r.nh, r.ny
    group = rows // 2

    def halo_copies(par):
        lo, hi = (nblk - 2) * cols_j, (nblk - 1) * cols_j
        return [
            remote(s0.at[lo:lo + cols_j], r.halo.at[par, 0], r.hsend.at[0], r.hrecv.at[par, 0], right),
            remote(s0.at[hi:hi + cols_j], r.halo.at[par, 1], r.hsend.at[1], r.hrecv.at[par, 1], left),
        ]

    def take_halo(par):
        for c in halo_copies(par):
            c.wait()
        low, high = r.halo[par, 0], r.halo[par, 1]
        low_w = jnp.concatenate([low[-1:], low[:-1]], axis=0)
        high_w = jnp.concatenate([high[1:], high[:1]], axis=0)
        r.edge_s[0] = jnp.where(me == 0, low_w, low)
        r.edge_s[1] = jnp.where(me == n - 1, high_w, high)

    def send(p, k, g):
        at = slice(SLAB * g, SLAB * g + SLAB)
        if k == 0:
            if p == nblk - 2:
                return r.edge_s[1, at, :]
            if p == nblk - 1:
                return r.keep[at, :]
            base = (p + 1) % nblk * cols_j
            return s0[base + SLAB * g:base + SLAB * g + SLAB, :]
        if k == 1:
            if p == nblk - 1:
                return r.edge_s[0, at, :]
            base = (p - 1) % nblk * cols_j
            return s0[base + SLAB * g:base + SLAB * g + SLAB, :]
        base = p * cols_j
        if k in (2, 3):
            return (sup, sdn)[k - 2][base + SLAB * g:base + SLAB * g + SLAB, :]
        sh = quarter if k == 4 else -quarter
        lo, hi = (SLAB * g + sh) % cols_j, (SLAB * g + 8 + sh) % cols_j
        return jnp.concatenate([s0[base + lo:base + lo + 8, :], s0[base + hi:base + hi + 8, :]], axis=0)

    def edge_act(i):
        for bb, p in enumerate(chunks[i]):
            for g in range(cols_j // SLAB):
                recv = rr[p * cols_j + SLAB * g:p * cols_j + SLAB * g + SLAB, :]
                for k in range(OFFSETS):
                    o = bb * per_blk + (g * OFFSETS + k) * SLAB
                    hid[i % 2][o:o + SLAB, :] = silu(pre[i % 2][o:o + SLAB, :] + send(p, k, g) + recv).astype(BF16)

    def edge_finish(i):
        rows6 = OFFSETS * SLAB
        for bb, p in enumerate(chunks[i]):
            for g in range(cols_j // SLAB):
                o = bb * per_blk + g * rows6
                eo = i * chunk + o
                new = (e[eo:eo + rows6, :].astype(F32) + layer_norm(ys[i % 2][o:o + rows6, :])).astype(BF16)
                e[eo:eo + rows6, :] = new
                total = new[0:SLAB].astype(F32)
                for k in range(1, OFFSETS):
                    total = total + new[k * SLAB:(k + 1) * SLAB].astype(F32)
                esum[p * cols_j + SLAB * g:p * cols_j + SLAB * g + SLAB, :] = total.astype(BF16)

    def edge_first(i, wi):
        pre[i % 2][0:chunk, :] = dot(e[i * chunk:(i + 1) * chunk, :], wi[0:latent, :])

    def edge_second(i, wo):
        ys[i % 2][0:chunk, :] = dot(hid[i % 2][0:chunk, :], wo[...])

    groups = ((0, group), (group, group // 2), (group + group // 2, group // 2))

    def project_send(g, wi):
        o, count = groups[g]
        s0[o:o + count, :] = dot(h[o:o + count, :], wi[latent:2 * latent, :])

    def roll_send(g):
        o, count = groups[g]
        for at in range(o, o + count, cols_j):
            blk = s0[at:at + cols_j, :]
            sup[at:at + cols_j, :] = jnp.concatenate([blk[1:], blk[:1]], axis=0)
            sdn[at:at + cols_j, :] = jnp.concatenate([blk[-1:], blk[:-1]], axis=0)

    def project_rest(g, wi, ni):
        o, count = groups[g]
        rr[o:o + count, :] = dot(h[o:o + count, :], wi[2 * latent:, :])
        n1[o:o + count, :] = dot(h[o:o + count, :], ni[0:latent, :])

    def node_first(g, ni):
        o, count = groups[g]
        npre[o:o + count, :] = dot(esum[o:o + count, :], ni[latent:, :])

    def node_act(g):
        o, count = groups[g]
        for at in range(o, o + count, SLAB):
            nhid[at:at + SLAB, :] = silu(npre[at:at + SLAB, :] + n1[at:at + SLAB, :]).astype(BF16)

    def node_second(g, no):
        o, count = groups[g]
        nys[o:o + count, :] = dot(nhid[o:o + count, :], no[...])

    def node_finish(g):
        o, count = groups[g]
        step = 4 * SLAB
        for at in range(o, o + count, step):
            h[at:at + step, :] = (h[at:at + step, :].astype(F32) + layer_norm(nys[at:at + step, :])).astype(BF16)

    def weights(i):
        return [x.at[i] for x in (r.lwi, r.lwo, r.lni, r.lno)]

    def layer_body(t, first):
        cur, was, nxt = (lax.rem(first + t + i, 3) for i in (0, 2, 1))
        par = lax.rem(first + t, 2)
        wi, wo, ni, no = weights(cur)
        wi_n, _, ni_n, _ = weights(nxt)
        _, wo_w, ni_w, no_w = weights(was)

        @pl.when(t > 0)
        def _():
            take_halo(1 - par)

        def run(stages, table):
            for stage in stages:
                name = stage.rstrip("0123456789")
                table[name](*(int(d) for d in stage[len(name):]))

        last_chunk = nchunk - 1
        run(LOWER, dict(
            A=edge_act, E=edge_finish, F=lambda i: edge_first(i, wi), S=lambda i: edge_second(i, wo_w if i == last_chunk else wo),
            nf=lambda g: node_first(g, ni_w), na=node_act, ns=lambda g: node_second(g, no_w), ne=node_finish,
            ps=lambda g: project_send(g, wi), ro=roll_send))
        for c in halo_copies(par):
            c.start()
        for c in fetch(jnp.where(t + 1 < layers, t + 2, 1), nxt):
            c.wait()
        for c in fetch(jnp.where(t + 2 < layers, t + 3, t + 3 - layers), was):
            c.start()

        def keep():
            r.keep[...] = s0[0:cols_j, :]

        run(UPPER, dict(
            A=edge_act, E=edge_finish, F=lambda i: edge_first(i, wi), S=lambda i: edge_second(i, wo),
            nf=lambda g: node_first(g, ni), na=node_act, ns=lambda g: node_second(g, no), ne=node_finish,
            ps=lambda g: project_send(g, wi if g else wi_n), pr=lambda g: project_rest(g, wi if g else wi_n, ni if g else ni_n), ro=roll_send, KEEP=keep))
        return first

    def run_layers(first):
        was, cur = (lax.rem(first + i, 3) for i in (2, 0))
        wi, _, ni, _ = weights(cur)
        r.lwo[was] = jnp.zeros((latent, latent), BF16)
        r.lno[was] = jnp.zeros((latent, latent), BF16)
        r.lni[was, latent:, :] = jnp.zeros((latent, latent), BF16)
        r.y0[...] = jnp.zeros(r.y0.shape, F32)
        project_send(0, wi)
        roll_send(0)
        project_rest(0, wi, ni)
        lax.fori_loop(0, layers, layer_body, first)
        was = lax.rem(first + layers + 2, 3)
        take_halo(lax.rem(first + layers + 1, 2))
        edge_act(7)
        edge_second(7, r.lwo.at[was])
        edge_finish(6)
        edge_finish(7)
        for g in (1, 2):
            node_first(g, r.lni.at[was])
            node_act(g)
            node_second(g, r.lno.at[was])
            node_finish(g)

    def step_body(s, _):
        x_prev, x_cur = r.xs.at[s], r.xs.at[1 - s]
        dmean, dstd = (r.ns[0:nvar, i:i + 1] for i in (2, 3))

        def self_body(q, _):
            base = pl.multiple_of(q * rows, rows)

            def first(w, u):
                r.p0[w, :] = dot(r.gl[pl.ds(base + u, half), :], r.wself[0])

            def second(w, u):
                r.y0[w, :] = dot(r.h0[w, :], r.wself[1])

            def store(o, v):
                w = pl.ds(base + o, GROUP)
                r.gcur[w, :] = (r.gl[w, :].astype(F32) + v).astype(BF16)

            chain(first, lambda w, u: act(r.p0, u, half, r.h0), second, lambda w, u: finish(r.y0, u, half, store))
            return 0

        lax.fori_loop(0, RATIO, self_body, 0)
        pl.when(s == 0)(late_static)

        def copy_body(i, _):
            at = pl.ds(pl.multiple_of(i * chunk, chunk), chunk)
            r.e[at, :] = r.ebase[at, :]
            return 0

        lax.fori_loop(0, nchunk, copy_body, 0)
        for q in range(2):
            for off in far_first:
                to_blocks(off, q, lax.rem(me + off, n), lax.rem(me + n - off, n)).wait()
        r.h[...] = dot(r.pfwd[...], r.hin[...].reshape(rows, latent)).astype(BF16)

        run_layers(s * layers)

        for q in range(2):
            r.yout[q] = dot(r.pbwd[q * half:(q + 1) * half, :], r.h[...]).astype(BF16).reshape(n, nblk, latent)
            for off in far_first:
                to_grid(off, q, lax.rem(me + off, n), me).start()
            r.hb[q, pl.ds(pl.multiple_of(nblk * me, nblk), nblk), :] = r.yout[q, me]

        def dec_body(q, _):
            base = pl.multiple_of(q * rows, rows)
            for off in far_first:
                to_grid(off, q, lax.rem(me + off, n), lax.rem(me + n - off, n)).wait()

            def edge_one(w, u):
                r.h1[w, :] = dot(r.ex[0:half, 0:half // RATIO], r.hb[q, u // RATIO:(u + half) // RATIO, :]).astype(BF16)
                r.p0[w, :] = dot(r.h1[w, :], r.wi[1, latent:2 * latent, :]) + dot(r.gcur[pl.ds(base + u, half), :], r.wi[1, 2 * latent:, :])

            def edge_two(w, u):
                r.y0[w, :] = dot(r.h0[w, :], r.wo[1])

            def store_edge(o, v):
                r.h1[o:o + GROUP, :] = (r.m2g[pl.ds(base + o, GROUP), :].astype(F32) + v).astype(BF16)

            def node_one(w, u):
                r.p1[w, :] = dot(r.gcur[pl.ds(base + u, half), :], r.ni[1, 0:latent, :]) + dot(r.h1[w, :], r.ni[1, latent:, :])

            def node_two(w, u):
                r.y1[w, :] = dot(r.h0[w, :], r.no[1])

            def store_node(o, v):
                r.h1[o:o + GROUP, :] = (r.gcur[pl.ds(base + o, GROUP), :].astype(F32) + v).astype(BF16)

            def out_one(w, u):
                r.p0[w, :] = dot(r.h1[w, :], r.woh[...])

            def out_two(w, u):
                at = pl.ds(pl.multiple_of(base + u, half), half)
                x_prev[:, at] = x_cur[:, at] + dstd * dot_bt(r.wof[...], r.h0[w, :]) + dmean

            chain(
                edge_one, lambda w, u: act(r.p0, u, half, r.h0, lambda o: r.decst[pl.ds(base + o, SLAB), :]),
                edge_two, lambda w, u: finish(r.y0, u, half, store_edge),
                node_one, lambda w, u: act(r.p1, u, half, r.h0),
                node_two, lambda w, u: finish(r.y1, u, half, store_node),
                out_one, lambda w, u: act(r.p0, u, half, r.h0), out_two,
            )

            @pl.when(s == 0)
            def _():
                grid_embed(1, base)
                encode(q)

            return 0

        lax.fori_loop(0, RATIO, dec_body, 0)
        for i, out in enumerate((r.out_a, r.out_b)):

            @pl.when(s == i)
            def _(i=i, out=out):
                pltpu.make_async_copy(r.xs.at[i], out, r.out_sem.at[i]).start()

        return 0

    for c in fetch(1, 0):
        c.wait()
    for c in fetch(2, 1):
        c.start()
    def first_encode(q, _):
        g2m_body(q)
        encode(q)
        return 0

    lax.fori_loop(0, RATIO, first_encode, 0)
    lax.fori_loop(0, 2, step_body, 0)
    for i, out in enumerate((r.out_a, r.out_b)):
        pltpu.make_async_copy(r.xs.at[i], out, r.out_sem.at[i]).wait()
    for c in fetch(1, (2 * layers + 1) % 3):
        c.wait()


def solution(mesh):
    n = mesh.shape["gp"]
    row_spec = P(("dp", "gp"))
    edge_spec = P(("dp", "gp"), None, None)
    whole = P()

    def local_run(x_prev, x_cur, forcing, grid_static, g2m_feat, m2g_feat, mesh_feat, mesh_edge_feat, norm_stats, w_grid_in, w_mesh_in, w_eemb_in, w_embed_out, w_edge_in, w_edge_out, w_node_in, w_node_out, w_grid_self, w_out_hidden, w_out_final):
        grid_rows, nvar = x_prev.shape
        rows = mesh_feat.shape[0]
        latent = w_embed_out.shape[-1]
        blocks = w_edge_in.shape[0]
        in_feat = w_grid_in.shape[0]
        shift = rows // 2
        cols_j = n * rows // shift
        nblk = shift // n
        chunk = 2 * OFFSETS * cols_j

        inputs = dict(xp_h=x_prev.T, xc_h=x_cur.T, fr_h=forcing.transpose(2, 1, 0), gs_h=grid_static.T, g2_h=g2m_feat.T, m2_h=m2g_feat.T, mf_h=mesh_feat.T, me_h=mesh_edge_feat.transpose(1, 2, 0), ns_h=norm_stats, wm_h=w_mesh_in, we_h=w_eemb_in, wg_h=w_grid_in, wemb_h=w_embed_out, wei_h=w_edge_in, weo_h=w_edge_out, wni_h=w_node_in, wno_h=w_node_out, wself_h=w_grid_self, woh_h=w_out_hidden, wof_h=w_out_final.T)
        big = max(rows, chunk)
        vm = pltpu.VMEM
        dma = pltpu.SemaphoreType.DMA
        scratch = dict(
            xs=vm((2, nvar, grid_rows), F32), fs=vm((2, 16, grid_rows), F32), ns=vm((256, 128), F32), gm=vm((2, 16, grid_rows), BF16), mf=vm((48, rows), BF16),
            ew=vm((4, 16, latent), BF16), wg=vm((rows, latent), BF16), wemb=vm(w_embed_out.shape, BF16),
            wi=vm((2, 3 * latent, latent), BF16), wo=vm((2, latent, latent), BF16), ni=vm((2, 2 * latent, latent), BF16), no=vm((2, latent, latent), BF16),
            wself=vm(w_grid_self.shape, BF16), woh=vm(w_out_hidden.shape, BF16),
            lwi=vm((3, 3 * latent, latent), BF16), lwo=vm((3, latent, latent), BF16), lni=vm((3, 2 * latent, latent), BF16), lno=vm((3, latent, latent), BF16),
            pfwd=vm((rows, rows), BF16), pbwd=vm((rows, rows), BF16), ex=vm((rows, rows // 2), BF16), ps=vm((rows // 2, rows), BF16),
            feat=vm((2, rows // 2, 128), BF16), fin=vm((cols_j, nblk, 128), BF16), featm=vm((rows, 128), BF16), mfp=vm((16, rows), BF16), g2p=vm((16, grid_rows), BF16),
            m2g=vm((grid_rows, latent), BF16), g2m=vm((grid_rows, latent), BF16), mlat=vm((rows, latent), BF16),
            decst=vm((grid_rows, latent), F32), encst=vm((grid_rows, latent), F32), nodst=vm((rows, latent), F32),
            gl=vm((grid_rows, latent), BF16), gcur=vm((grid_rows, latent), BF16), mcur=vm((2, rows // 2, latent), BF16),
            hin=vm((cols_j, nblk, latent), BF16), hb=vm((2, rows // 2, latent), BF16), yout=vm((2, n, nblk, latent), BF16),
            ebase=vm((OFFSETS * rows, latent), BF16), e=vm((OFFSETS * rows, latent), BF16), h=vm((rows, latent), BF16),
            s0=vm((rows, latent), F32), sup=vm((rows, latent), F32), sdn=vm((rows, latent), F32), rr=vm((rows, latent), F32), n1=vm((rows, latent), F32),
            esum=vm((rows, latent), BF16), edge_s=vm((2, cols_j, latent), F32), keep=vm((cols_j, latent), F32), np=vm((rows, latent), F32), nh=vm((rows, latent), BF16), ny=vm((rows, latent), F32), halo=vm((2, 2, cols_j, latent), F32),
            p0=vm((big, latent), F32), p1=vm((big, latent), F32), h0=vm((big, latent), BF16), h1=vm((big, latent), BF16), y0=vm((big, latent), F32), y1=vm((big, latent), F32),
            wof=vm((nvar, latent), BF16), mfr=vm((mesh_feat.shape[1], rows), F32), mer=vm((*mesh_edge_feat.shape[1:], rows), F32), g2r=vm((g2m_feat.shape[1], grid_rows), F32), m2r=vm((m2g_feat.shape[1], grid_rows), F32),
            gsr=vm((grid_static.shape[1], grid_rows), F32), frr=vm((forcing.shape[2], forcing.shape[1], grid_rows), F32), nsr=vm(norm_stats.shape, F32), wmr=vm(w_mesh_in.shape, BF16), wer=vm(w_eemb_in.shape, BF16),
            load_sem=dma((24,)), fetch_sem=dma((3, 4)), out_sem=dma((2,)), fsend=dma((n,)), frecv=dma((n,)), nsend=dma((2,)), nrecv=dma((2,)),
            asend=dma((n, 2)), arecv=dma((n, 2)), bsend=dma((n, 2)), brecv=dma((n, 2)), hsend=dma((2,)), hrecv=dma((2, 2)),
        )
        cfg = types.SimpleNamespace(names=(*inputs, "out_a", "out_b", *scratch), n=n, rows=rows, latent=latent, shift=shift, layers=blocks - 2, nvar=nvar, in_feat=in_feat)
        anywhere = pl.BlockSpec(memory_space=pl.ANY)
        out = pl.pallas_call(
            functools.partial(kernel, cfg),
            out_shape=[jax.ShapeDtypeStruct((nvar, grid_rows), F32)] * 2,
            in_specs=[anywhere] * len(inputs),
            out_specs=[anywhere] * 2,
            scratch_shapes=list(scratch.values()),
            compiler_params=pltpu.CompilerParams(collective_id=0, has_side_effects=True, vmem_limit_bytes=66_000_000),
        )(*inputs.values())
        return out[0].T, out[1].T

    in_specs = (row_spec, row_spec, edge_spec, row_spec, row_spec, row_spec, row_spec, edge_spec, whole) + (whole,) * 11
    return jax.shard_map(local_run, mesh=mesh, in_specs=in_specs, out_specs=(row_spec, row_spec), check_vma=False)
```
